128 devices in a mesh: grid: 8 (over x, y_lo), row: 8 (over z, core), rhs: 2 (over y_hi).
Axes of the slice: x: 4, y: 4 (y_hi: 2, y_lo: 2; y = y_hi * 2 + y_lo), z: 4, core: 2. Of those that a mesh axis runs over, the one named last changes fastest.
Arguments:
- leaf_rhs: float32 [49152, 2048], P(('grid', 'row'), 'rhs'), parts along dimension 1, may hold values from -6 to 6
- block_sizes: int32 [64], P(('grid', 'row')), may hold values from 384 to 768, as said below
- leaf_lower: float32 [49152, 256], P(('grid', 'row')), may hold values from -0.25 to 0.25
- leaf_inverse: float32 [49152, 768], P(('grid', 'row')), as said below
- coupling: float32 [32768, 768], P(('grid', 'row')), may hold values from -0.02734375 to 0.02734375
- anc_rows: int32 [32768], P(('grid', 'row')), may hold values from 0 to 767, as said below
- anc_rhs: float32 [768, 2048], P(None, 'rhs'), parts along dimension 1, may hold values from -6 to 6
- anc_inverse: float32 [768, 768], replicated, as said below
Outputs:
- leaf_solution: float32 [49152, 2048], P(('grid', 'row'), 'rhs'), parts along dimension 1
- anc_solution: float32 [768, 2048], P('row', 'rhs'), parts along dimension 1
The draws below stay inside these ranges and needn't reach their ends.
There are 2 independent parts, one for each index of `rhs`. The reference program is written for one: setup_inputs(seed, part) draws one part's arguments, and reference() takes and returns one part's arrays. A program takes and returns all parts, laid end to end along the dimension named above; an argument that names none is the same for every part. Nothing has to cross between parts.
Inputs may be any that keep to these rules, and one draw needn't show every extreme that they name: `block_sizes`: every value lies between 384 and 768; some block row uses all 768 rows and another exactly 384. `anc_rows`: within each block row's 512 entries the ancestor rows are distinct and increasing. `leaf_inverse`: each 768 x 768 block is lower triangular with a unit diagonal. `anc_inverse`: lower triangular with a unit diagonal.
All inputs are finite; a program needn't handle non-finite values.
Results may differ from the reference program's by a relative error of at most 0.0001.
Values sent between devices are 32-bit elements; how exact they have to be, the bound alone decides.
No kernel may reach another device: no remote copies, remote signals or barrier semaphores. Data moves between devices by JAX's collectives and lax.ppermute only.
A program may use at most 128 MiB of HBM per device.

```python
import jax
import jax.numpy as jnp
from jax import lax

BS = 768
LR = 256
CR = 512
ANC = 768
NRHS = 1024
NBLK = 64
N_GRID = 8
N_ROW = 8


def unit_lower(key, count, order):
    key_one = jax.random.fold_in(key, 0)
    gauss = jax.random.normal(key_one, (count, order, order), jnp.float32)
    strict = jnp.tril(gauss, -1) * (0.7 / jnp.sqrt(jnp.float32(order)))
    return strict + jnp.eye(order, dtype=jnp.float32)[None]


def draw_leaf_inverse(key, part):
    mine = jax.random.fold_in(key, 11)
    return unit_lower(mine, NBLK, BS).reshape(NBLK * BS, BS)


def draw_anc_inverse(key, part):
    mine = jax.random.fold_in(key, 13)
    return unit_lower(mine, 1, ANC).reshape(ANC, ANC)


def draw_block_sizes(key, part):
    mine = jax.random.fold_in(key, 17)
    key_one, key_two = jax.random.split(mine)
    sizes = jax.random.randint(key_one, (NBLK,), BS // 2, BS + 1, dtype=jnp.int32)
    chosen = jax.random.randint(key_two, (), 0, NBLK, dtype=jnp.int32)
    places = jnp.arange(NBLK, dtype=jnp.int32)
    sizes = jnp.where(places == chosen, BS, sizes)
    sizes = jnp.where(places == (chosen + 1) % NBLK, BS // 2, sizes)
    return sizes.astype(jnp.int32)


def draw_anc_rows(key, part):
    mine = jax.random.fold_in(key, 19)
    keys = jax.random.split(mine, NBLK)

    def pick(single):
        return jnp.sort(jax.random.permutation(single, ANC)[:CR])
    return jax.vmap(pick)(keys).reshape(NBLK * CR).astype(jnp.int32)


def steps_of(stream_key, shape, cuts, low, top_value):
    factor_of, own = 1.0, jax.random.fold_in(stream_key, 6)
    for dim, parts in cuts:
        heights = jnp.exp(jax.random.uniform(jax.random.fold_in(own, dim), (parts,), jnp.float32, low / len(cuts), top_value / len(cuts)))
        factor_of = factor_of * jnp.repeat(heights, shape[dim] // parts).reshape([-1 if axis == dim else 1 for axis in range(len(shape))])
    return factor_of


def noise(stream_key, extent, spread, bound, cuts=(), kind=jnp.bfloat16):
    values = jax.random.normal(stream_key, extent, jnp.float32) * spread
    if len(cuts) > 0:
        values = steps_of(stream_key, extent, cuts, -0.22, 0.18) * values
    return jnp.clip(values, min=-bound, max=bound).astype(kind)


def setup_inputs(seed: int = 0, part: int = 0) -> dict:
    streams_of = jax.random.split(jax.random.key(seed), 9)
    own_keys = jax.random.split(jax.random.fold_in(streams_of[8], part), 9)
    return {
        "leaf_rhs": noise(own_keys[0], (NBLK * BS, NRHS), 1.0, 6.0, ((0, 64),), jnp.float32),
        "block_sizes": draw_block_sizes(jax.random.fold_in(streams_of[8], 71), part),
        "leaf_lower": noise(streams_of[2], (NBLK * BS, LR), (2 * LR) ** -0.5, 0.25, ((0, 64),), jnp.float32),
        "leaf_inverse": draw_leaf_inverse(jax.random.fold_in(streams_of[8], 71), part),
        "coupling": noise(streams_of[4], (NBLK * CR, BS), (BS * NBLK) ** -0.5, 0.02734375, ((0, 64),), jnp.float32),
        "anc_rows": draw_anc_rows(jax.random.fold_in(streams_of[8], 71), part),
        "anc_rhs": noise(own_keys[6], (ANC, NRHS), 1.0, 6.0, (), jnp.float32),
        "anc_inverse": draw_anc_inverse(jax.random.fold_in(streams_of[8], 71), part),
    }


def reference(leaf_rhs, block_sizes, leaf_lower, leaf_inverse, coupling, anc_rows, anc_rhs, anc_inverse):
    highest = lax.Precision.HIGHEST
    blocks_all = N_GRID * N_ROW
    right_blocks = leaf_rhs.reshape(N_GRID, N_ROW, BS, NRHS)
    lower_blocks = leaf_lower.reshape(N_GRID, N_ROW, BS, LR)
    inverses = leaf_inverse.reshape(N_GRID, N_ROW, BS, BS)
    live_rows = (jnp.arange(BS, dtype=jnp.int32)[None, None, :] < block_sizes.reshape(N_GRID, N_ROW)[:, :, None]).astype(jnp.float32)
    carried = jnp.zeros((N_GRID, LR, NRHS), jnp.float32)
    solved_blocks = []
    for level in range(N_ROW):
        reduced = right_blocks[:, level] - jnp.einsum('gbl,gln->gbn', lower_blocks[:, level], carried, precision=highest)
        solved = jnp.einsum('gab,gbn->gan', inverses[:, level], reduced, precision=highest) * live_rows[:, level, :, None]
        solved_blocks.append(solved)
        carried = solved[:, :LR]
    leaf_solution = jnp.stack(solved_blocks, axis=1).reshape(blocks_all * BS, NRHS)
    coupled = jnp.einsum('kcb,kbn->kcn', coupling.reshape(blocks_all, CR, BS), leaf_solution.reshape(blocks_all, BS, NRHS), precision=highest).reshape(blocks_all * CR, NRHS)
    partial_value = jnp.zeros((ANC, NRHS), jnp.float32).at[anc_rows].add(coupled)
    anc_solution = jnp.dot(anc_inverse, anc_rhs - partial_value, precision=highest, preferred_element_type=jnp.float32)
    return leaf_solution, anc_solution
```

```python
import functools

import jax
import jax.numpy as jnp
from jax import lax
from jax.experimental import pallas as pl
from jax.experimental.pallas import tpu as pltpu
from jax.sharding import Mesh
from jax.sharding import PartitionSpec as P

F32 = jnp.float32
BF16 = jnp.bfloat16
GRID_ROW = ("x", "yl", "z", "core")


def shifted(array, axis, by, sources=None):
    devices = lax.axis_size(axis)
    pairs = [(i, (i + by) % devices) for i in range(devices)]
    if sources is not None:
        pairs = [pair for pair in pairs if pair[0] in sources]
    return lax.ppermute(array, axis, pairs)


def halves(a):
    high = a.astype(BF16)
    return high, (a - high.astype(F32)).astype(BF16)


def mxu(a, b):
    return jnp.dot(a, b, preferred_element_type=F32)


def dot3(a, b):
    return mxu(a[0], b[0]) + (mxu(a[0], b[1]) + mxu(a[1], b[0]))


def flops(m, k, n):
    return 6 * m * k * n


def cost(n_flops, n_bytes):
    return pl.CostEstimate(flops=n_flops, transcendentals=0, bytes_accessed=n_bytes)


SMEM = pl.BlockSpec(memory_space=pltpu.SMEM)


def call(kernel, outs, scratch=(), n_flops=1 << 20, in_specs=None, name=None):
    return pl.pallas_call(
        kernel,
        out_shape=[jax.ShapeDtypeStruct(s, F32) for s in outs],
        in_specs=in_specs,
        scratch_shapes=list(scratch),
        cost_estimate=cost(n_flops, 1 << 20),
        name=name,
    )


def lead_kernel(place, size, inverse, lower, rhs, a_out, keep_out, send_out):
    rows = lax.broadcasted_iota(jnp.int32, inverse.shape, 0)
    s = halves(jnp.where(rows < size[0], inverse[...], 0.0))
    a_out[...] = dot3(s, halves(lower[...]))
    half = rhs.shape[1] // 2
    first = dot3(s, halves(rhs[:, :half]))
    second = dot3(s, halves(rhs[:, half:]))
    own_first = place[1] == 0
    keep_out[...] = jnp.where(own_first, first, second)
    send_out[...] = jnp.where(own_first, second, first)


def merge_kernel(place, a_own, a_other, b_own, b_other, o0, o1, o2, o3, a_out, quarters):
    z, low = place[0], place[1] == 0
    a_low = jnp.where(low, a_own[...], a_other[...])
    a_high = halves(jnp.where(low, a_other[...], a_own[...]))
    b_low = jnp.where(low, b_own[...], b_other[...])
    b_high = jnp.where(low, b_other[...], b_own[...])
    a_out[...] = dot3(a_high, halves(a_low))
    merged = b_high - dot3(a_high, halves(b_low))
    count, _, width = quarters.shape
    for i in range(count):
        quarters[i] = merged[:, i * width : (i + 1) * width]
    for s, out in enumerate((o0, o1, o2, o3)):
        out[...] = quarters[lax.rem(z + s, count)]


def solve_kernel(place, r0, r1, r2, r3, a0, a1, a2, a3, o0, o1, o2, o3, bs, mats, ends):
    z = place[0]
    count = bs.shape[0]
    for s, (r, a) in enumerate(((r0, a0), (r1, a1), (r2, a2), (r3, a3))):
        at = lax.rem(z + count - s, count)
        bs[at] = r[...]
        mats[at] = a[...]
    ends[0] = jnp.zeros(ends.shape[1:], F32)
    carried = bs[0]
    ends[1] = carried
    for i in range(1, count - 1):
        carried = bs[i] + dot3(halves(mats[i]), halves(carried))
        ends[i + 1] = carried
    for s, out in enumerate((o0, o1, o2, o3)):
        out[...] = ends[lax.rem(z + s, count)]


def gather_kernel(place, t0, t1, t2, t3, a_own, a_other, b_own, b_other, keep, send, quarters):
    z, low = place[0], place[1] == 0
    count = quarters.shape[0]
    for s, t in enumerate((t0, t1, t2, t3)):
        quarters[lax.rem(z + count - s, count)] = t[...]
    a_low = halves(jnp.where(low, a_own[...], a_other[...]))
    width = quarters.shape[2]
    for i in range(count):
        cols = slice(i * width, (i + 1) * width)
        end = quarters[i]
        b_low = jnp.where(low, b_own[:, cols], b_other[:, cols])
        middle = b_low - dot3(a_low, halves(end))
        keep[:, cols] = jnp.where(low, end, middle)
        send[:, cols] = jnp.where(low, middle, end)


def finish_kernel(place, own, other, h, n, f, c, sol, keep, send, hh, hl, nh, nl):
    step = pl.program_id(0)

    @pl.when(step == 0)
    def _():
        hh[...], hl[...] = halves(h[...])
        nh[...], nl[...] = halves(n[...])

    low = place[1] == 0
    mine = (step // 2) == place[1]
    carried = halves(jnp.where(mine, own[...], other[...]))
    sol[...] = f[...] - dot3((hh[...], hl[...]), carried)
    y = c[...] - dot3((nh[...], nl[...]), carried)
    groups, planes, share, width = keep.shape
    for g in range(groups):
        cols = slice(g * width, (g + 1) * width)
        for p in range(planes):
            top = y[2 * p * share : (2 * p + 1) * share, cols]
            bottom = y[(2 * p + 1) * share : (2 * p + 2) * share, cols]
            keep[g, p] = jnp.where(low, top, bottom)
            send[g, p] = jnp.where(low, bottom, top)


def body(leaf_rhs, block_sizes, leaf_lower, leaf_inverse, coupling, anc_rows, anc_rhs, anc_inverse):
    high = functools.partial(jnp.dot, precision=lax.Precision.HIGH, preferred_element_type=F32)
    rows, columns = leaf_rhs.shape
    lead = leaf_lower.shape[1]
    anc = anc_inverse.shape[0]
    planes, cores = lax.axis_size("z"), lax.axis_size("core")
    groups = lax.axis_size("x") * lax.axis_size("yl")
    z, core = lax.axis_index("z"), lax.axis_index("core")
    place = jnp.stack([z, core]).astype(jnp.int32)
    half, quarter = columns // cores, columns // (cores * planes)
    share, width = anc // (planes * cores), columns // groups

    block = lambda r, c: pl.BlockSpec((r, c), lambda i: (0, 0))
    a_own, b_own, b_send = pl.pallas_call(
        lead_kernel,
        grid=(1,),
        in_specs=[SMEM, SMEM, block(lead, lead), block(lead, lead), block(lead, columns)],
        out_specs=[block(lead, lead), block(lead, half), block(lead, half)],
        out_shape=[jax.ShapeDtypeStruct((lead, w), F32) for w in (lead, half, half)],
        cost_estimate=cost(flops(lead, lead, lead + columns), 1 << 21),
        name="lead",
    )(place, block_sizes, leaf_inverse, leaf_lower, leaf_rhs)
    a_other = shifted(a_own, "core", 1)
    b_other = shifted(b_send, "core", 1)

    vm = pl.BlockSpec(memory_space=pltpu.VMEM)
    piece, square = (lead, quarter), (lead, lead)
    *blocks, a_pair = call(
        merge_kernel,
        [piece] * 4 + [square],
        [pltpu.VMEM((planes, *piece), F32)],
        flops(lead, lead, half + lead),
        [SMEM] + [vm] * 4,
        "merge",
    )(place, a_own, a_other, b_own, b_other)
    mats = [a_pair] + [shifted(a_pair, "z", s, (1, 2)) for s in range(1, planes)]
    blocks = [blocks[0]] + [shifted(blocks[s], "z", s, (0, 1, 2)) for s in range(1, planes)]
    ends = call(
        solve_kernel,
        [piece] * 4,
        [
            pltpu.VMEM((planes, *piece), F32),
            pltpu.VMEM((planes, *square), F32),
            pltpu.VMEM((planes, *piece), F32),
        ],
        flops(lead, lead, 2 * quarter),
        [SMEM] + [vm] * 8,
        "solve",
    )(place, *blocks, *mats)
    ends = [ends[0]] + [shifted(ends[s], "z", s) for s in range(1, planes)]
    own, passed = call(
        gather_kernel,
        [(lead, half)] * 2,
        [pltpu.VMEM((planes, *piece), F32)],
        flops(lead, lead, half),
        [SMEM] + [vm] * 8,
        "gather",
    )(place, *ends, a_own, a_other, b_own, b_other)
    other = shifted(passed, "core", 1)

    live = (jnp.arange(rows, dtype=jnp.int32) < block_sizes[0]).astype(F32)
    scaled = leaf_inverse * live[:, None]
    f = high(scaled, leaf_rhs)
    h = high(scaled, leaf_lower)
    one_hot = (jnp.arange(anc, dtype=jnp.int32)[:, None] == anc_rows[None, :]).astype(F32)
    m = high(high(anc_inverse, one_hot), coupling)
    c = high(m, f)
    n = high(m, h)

    step = 2 * width
    tall = pl.BlockSpec((rows, step), lambda j: (0, j))
    part = pl.BlockSpec((lead, step), lambda j: (0, lax.rem(j, half // step)))
    whole = pl.BlockSpec((rows, lead), lambda j: (0, 0))
    blocked = pl.BlockSpec((step // width, planes, share, width), lambda j: (j, 0, 0, 0))
    sol, keep, send = pl.pallas_call(
        finish_kernel,
        grid=(columns // step,),
        in_specs=[SMEM, part, part, whole, whole, tall, tall],
        out_specs=[tall, blocked, blocked],
        out_shape=[jax.ShapeDtypeStruct((rows, columns), F32)]
        + [jax.ShapeDtypeStruct((groups, planes, share, width), F32)] * 2,
        scratch_shapes=[pltpu.VMEM((rows, lead), BF16)] * 4,
        cost_estimate=cost(flops(2 * rows, lead, columns), 1 << 23),
        name="finish",
    )(place, own, other, h, n, f, c)

    summed = keep + shifted(send, "core", 1)
    arrived = lax.all_to_all(
        summed.reshape(groups * planes, share, width), ("x", "yl", "z"), 0, 0, tiled=True
    )
    group = lax.axis_index(("x", "yl"))
    own_rows = lax.dynamic_slice_in_dim(anc_inverse, (z * cores + core) * share, share, 0)
    own_cols = lax.dynamic_slice_in_dim(anc_rhs, group * width, width, 1)
    anc_block = high(own_rows, own_cols) - jnp.sum(arrived, axis=0)
    spread = lax.all_to_all(
        jnp.broadcast_to(anc_block[None], (groups, share, width)), ("x", "yl"), 0, 0, tiled=True
    )
    return sol, jnp.moveaxis(spread, 0, 1).reshape(share, columns)


def solution(mesh):
    split = Mesh(
        mesh.devices.reshape(4, 2, 4, 2, mesh.shape["rhs"]), ("x", "yl", "z", "core", "rhs")
    )
    in_specs = (
        P(GRID_ROW, "rhs"),
        P(GRID_ROW),
        P(GRID_ROW, None),
        P(GRID_ROW, None),
        P(GRID_ROW, None),
        P(GRID_ROW),
        P(None, "rhs"),
        P(),
    )
    out_specs = (P(GRID_ROW, "rhs"), P(("z", "core"), "rhs"))
    return jax.shard_map(body, mesh=split, in_specs=in_specs, out_specs=out_specs, check_vma=False)
```

```python
import jax
import jax.numpy as jnp
from jax import lax
from jax.experimental import pallas as pl
from jax.experimental.pallas import tpu as pltpu
from jax.sharding import Mesh
from jax.sharding import PartitionSpec as P

F32 = jnp.float32
BF16 = jnp.bfloat16
GRID_ROW = ("x", "yl", "z", "core")


def shifted(array, axis, by, sources=None):
    devices = lax.axis_size(axis)
    pairs = [(i, (i + by) % devices) for i in range(devices)]
    if sources is not None:
        pairs = [pair for pair in pairs if pair[0] in sources]
    return lax.ppermute(array, axis, pairs)


def halves(a):
    high = a.astype(BF16)
    return high, (a - high.astype(F32)).astype(BF16)


def mxu(a, b):
    return jnp.dot(a, b, preferred_element_type=F32)


def dot3(a, b):
    return mxu(a[0], b[0]) + (mxu(a[0], b[1]) + mxu(a[1], b[0]))


def flops(m, k, n):
    return 6 * m * k * n


def cost(n_flops, n_bytes):
    return pl.CostEstimate(flops=n_flops, transcendentals=0, bytes_accessed=n_bytes)


SMEM = pl.BlockSpec(memory_space=pltpu.SMEM)
VMEM = pl.BlockSpec(memory_space=pltpu.VMEM)


def near(array):
    return pltpu.with_memory_space_constraint(array, pltpu.VMEM)


def small(kernel, name, place, arrays, outs, scratch=(), n_flops=1 << 20):
    return pl.pallas_call(
        kernel,
        in_specs=[SMEM] + [VMEM] * len(arrays),
        out_specs=[VMEM] * len(outs),
        out_shape=[pltpu.VMEM(shape, F32) for shape in outs],
        scratch_shapes=list(scratch),
        cost_estimate=cost(n_flops, 1 << 20),
        name=name,
    )(place, *[near(a) for a in arrays])


def lead_kernel(place, size, inverse, lower, rhs, a_out, keep_out, send_out):
    rows = lax.broadcasted_iota(jnp.int32, inverse.shape, 0)
    s = halves(jnp.where(rows < size[0], inverse[...], 0.0))
    a_out[...] = dot3(s, halves(lower[...]))
    half = rhs.shape[1] // 2
    first = dot3(s, halves(rhs[:, :half]))
    second = dot3(s, halves(rhs[:, half:]))
    own_first = place[1] == 0
    keep_out[...] = jnp.where(own_first, first, second)
    send_out[...] = jnp.where(own_first, second, first)


def merge_kernel(place, a_own, a_other, b_own, b_other, o0, o1, o2, o3, a_out, quarters):
    z, low = place[0], place[1] == 0
    a_low = jnp.where(low, a_own[...], a_other[...])
    a_high = halves(jnp.where(low, a_other[...], a_own[...]))
    b_low = jnp.where(low, b_own[...], b_other[...])
    b_high = jnp.where(low, b_other[...], b_own[...])
    a_out[...] = dot3(a_high, halves(a_low))
    merged = b_high - dot3(a_high, halves(b_low))
    count, _, width = quarters.shape
    for i in range(count):
        quarters[i] = merged[:, i * width : (i + 1) * width]
    for s, out in enumerate((o0, o1, o2, o3)):
        out[...] = quarters[lax.rem(z + s, count)]


def solve_kernel(place, r0, r1, r2, r3, a0, a1, a2, a3, o0, o1, o2, o3, bs, mats, ends):
    z = place[0]
    count = bs.shape[0]
    for s, (r, a) in enumerate(((r0, a0), (r1, a1), (r2, a2), (r3, a3))):
        at = lax.rem(z + count - s, count)
        bs[at] = r[...]
        mats[at] = a[...]
    ends[0] = jnp.zeros(ends.shape[1:], F32)
    carried = bs[0]
    ends[1] = carried
    for i in range(1, count - 1):
        carried = bs[i] + dot3(halves(mats[i]), halves(carried))
        ends[i + 1] = carried
    for s, out in enumerate((o0, o1, o2, o3)):
        out[...] = ends[lax.rem(z + s, count)]


def gather_kernel(place, t0, t1, t2, t3, out, quarters):
    z = place[0]
    count, _, width = quarters.shape
    for s, t in enumerate((t0, t1, t2, t3)):
        quarters[lax.rem(z + count - s, count)] = t[...]
    for i in range(count):
        out[:, i * width : (i + 1) * width] = quarters[i]


def weigh_kernel(rows, inverse, coupling, m_high, m_low, hot):
    anc, touched = hot.shape
    at = lax.broadcasted_iota(jnp.int32, (anc, touched), 0)
    hot[...] = jnp.where(at == rows[...], 1.0, 0.0).astype(BF16)
    right = halves(coupling[...])
    block = anc // 3
    for i in range(3):
        span = slice(i * block, (i + 1) * block)
        reach, cols = (i + 1) * block, min(touched, (i + 1) * block)
        high, low = halves(inverse[span, :reach])
        picked = hot[:reach, :cols]
        g = halves(mxu(high, picked) + mxu(low, picked))
        m = dot3(g, tuple(part[:cols] for part in right))
        m_high[span], m_low[span] = halves(m)


def leaf_kernel(place, size, inverse, lower, rhs, b_first, b_second, a_low, out, sh, sl, lh, ll, t):
    step, last = pl.program_id(0), pl.num_programs(0) - 1
    high_core = place[1] == 1

    @pl.when(step == 0)
    def _():
        rows = lax.broadcasted_iota(jnp.int32, inverse.shape, 0)
        sh[...], sl[...] = halves(jnp.where(rows < size[0], inverse[...], 0.0))
        lh[...], ll[...] = halves(lower[...])

    @pl.when(step < last)
    def _():
        entering = jnp.where(step < last // 2, b_first[...], b_second[...])
        entering = jnp.where(high_core, entering, 0.0)
        t[...] = rhs[...] - dot3((lh[...], ll[...]), halves(entering))

    @pl.when(step == last)
    def _():
        t[...] = jnp.where(
            high_core, -dot3((lh[...], ll[...]), halves(a_low[...])), lower[...]
        )

    right = halves(t[...])
    block = inverse.shape[0] // 3
    for i in range(3):
        span, reach = slice(i * block, (i + 1) * block), (i + 1) * block
        out[span] = dot3((sh[span, :reach], sl[span, :reach]), (right[0][:reach], right[1][:reach]))


def by_owner(place, value, keep, send):
    low = place[1] == 0
    groups, planes, share, width = keep.shape
    for g in range(groups):
        cols = slice(g * width, (g + 1) * width)
        for p in range(planes):
            top = value[2 * p * share : (2 * p + 1) * share, cols]
            bottom = value[(2 * p + 1) * share : (2 * p + 2) * share, cols]
            keep[g, p] = jnp.where(low, top, bottom)
            send[g, p] = jnp.where(low, bottom, top)


def couple_kernel(place, m_high, m_low, leaf, keep, send):
    by_owner(place, dot3((m_high[...], m_low[...]), halves(leaf[...])), keep, send)


def update_kernel(place, own, other, n_keep, n_other, c_keep, c_other, out, nh, nl):
    step = pl.program_id(0)
    groups, planes, share, width = out.shape
    tall = planes * share

    @pl.when(step == 0)
    def _():
        for g in range(groups):
            n = (n_keep[g] + n_other[g]).reshape(tall, width)
            cols = slice(g * width, (g + 1) * width)
            nh[:, cols], nl[:, cols] = halves(n)

    mine = (step // 2) == place[1]
    carried = halves(jnp.where(mine, own[...], other[...]))
    moved = dot3((nh[...], nl[...]), carried)
    for g in range(groups):
        c = (c_keep[g] + c_other[g]).reshape(tall, width)
        out[g] = (c - moved[:, g * width : (g + 1) * width]).reshape(planes, share, width)


def finish_kernel(place, own, other, h, f, sol, hh, hl):
    step = pl.program_id(0)

    @pl.when(step == 0)
    def _():
        hh[...], hl[...] = halves(h[...])

    mine = (step // 2) == place[1]
    carried = halves(jnp.where(mine, own[...], other[...]))
    sol[...] = f[...] - dot3((hh[...], hl[...]), carried)


def total_kernel(own_rows, own_cols, arrived, out):
    total = arrived[0]
    for i in range(1, arrived.shape[0]):
        total = total + arrived[i]
    out[...] = dot3(halves(own_rows[...]), halves(own_cols[...])) - total


def body(leaf_rhs, block_sizes, leaf_lower, leaf_inverse, coupling, anc_rows, anc_rhs, anc_inverse):
    rows, columns = leaf_rhs.shape
    lead = leaf_lower.shape[1]
    anc, touched = anc_inverse.shape[0], anc_rows.shape[0]
    planes, cores = lax.axis_size("z"), lax.axis_size("core")
    groups = lax.axis_size("x") * lax.axis_size("yl")
    z, core = lax.axis_index("z"), lax.axis_index("core")
    place = jnp.stack([z, core]).astype(jnp.int32)
    half, quarter = columns // cores, columns // (cores * planes)
    share, width = anc // (planes * cores), columns // groups
    piece, square = (lead, quarter), (lead, lead)

    block = lambda r, c: pl.BlockSpec((r, c), lambda i: (0, 0))
    a_own, b_own, b_send = pl.pallas_call(
        lead_kernel,
        grid=(1,),
        in_specs=[SMEM, SMEM, block(lead, lead), block(lead, lead), block(lead, columns)],
        out_specs=[VMEM] * 3,
        out_shape=[pltpu.VMEM((lead, w), F32) for w in (lead, half, half)],
        cost_estimate=cost(flops(lead, lead, lead + columns), 1 << 21),
        name="lead",
    )(place, block_sizes, leaf_inverse, leaf_lower, leaf_rhs)
    a_other = shifted(a_own, "core", 1)
    b_other = shifted(b_send, "core", 1)
    b_low = shifted(b_own, "core", 1, (0,))

    m_high, m_low = pl.pallas_call(
        weigh_kernel,
        out_shape=[jax.ShapeDtypeStruct((anc, rows), BF16)] * 2,
        scratch_shapes=[pltpu.VMEM((anc, touched), BF16)],
        cost_estimate=cost(flops(anc, touched, rows + anc), 1 << 22),
        name="weigh",
    )(anc_rows[None], anc_inverse, coupling)

    *blocks, a_pair = small(
        merge_kernel,
        "merge",
        place,
        (a_own, a_other, b_own, b_other),
        [piece] * 4 + [square],
        [pltpu.VMEM((planes, *piece), F32)],
        flops(lead, lead, half + lead),
    )
    mats = [a_pair] + [shifted(a_pair, "z", s, (1, 2)) for s in range(1, planes)]
    blocks = [blocks[0]] + [shifted(blocks[s], "z", s, (0, 1, 2)) for s in range(1, planes)]

    step = 2 * width
    steps = columns // step
    whole = lambda r, c: pl.BlockSpec((r, c), lambda j: (0, 0))
    part = pl.BlockSpec((lead, step), lambda j: (0, lax.rem(j, half // step)))
    tall = pl.BlockSpec((rows, step), lambda j: (0, j))
    leaf = pl.pallas_call(
        leaf_kernel,
        grid=(steps + 1,),
        in_specs=[
            SMEM,
            SMEM,
            whole(rows, rows),
            whole(rows, lead),
            pl.BlockSpec((rows, step), lambda j: (0, jnp.minimum(j, steps - 1))),
            part,
            part,
            whole(*square),
        ],
        out_specs=tall,
        out_shape=jax.ShapeDtypeStruct((rows, columns + lead), F32),
        scratch_shapes=[pltpu.VMEM((rows, rows), BF16)] * 2
        + [pltpu.VMEM((rows, lead), BF16)] * 2
        + [pltpu.VMEM((rows, step), F32)],
        cost_estimate=cost(flops(rows, rows, columns), 1 << 23),
        name="leaf",
    )(place, block_sizes, leaf_inverse, leaf_lower, leaf_rhs, b_low, b_other, a_other)
    blocked = pl.BlockSpec((step // width, planes, share, width), lambda j: (j, 0, 0, 0))
    wide = (columns + lead) // width
    keep, send = pl.pallas_call(
        couple_kernel,
        grid=(steps + 1,),
        in_specs=[SMEM, whole(anc, rows), whole(anc, rows), tall],
        out_specs=[blocked, blocked],
        out_shape=[jax.ShapeDtypeStruct((wide, planes, share, width), F32)] * 2,
        cost_estimate=cost(flops(anc, rows, columns + lead), 1 << 23),
        name="couple",
    )(place, m_high, m_low, leaf)
    keep_other = shifted(send, "core", 1)

    ends = small(
        solve_kernel,
        "solve",
        place,
        (*blocks, *mats),
        [piece] * 4,
        [
            pltpu.VMEM((planes, *piece), F32),
            pltpu.VMEM((planes, *square), F32),
            pltpu.VMEM((planes, *piece), F32),
        ],
        flops(lead, lead, 2 * quarter),
    )
    ends = [ends[0]] + [shifted(ends[s], "z", s) for s in range(1, planes)]
    (own,) = small(
        gather_kernel, "gather", place, ends, [(lead, half)], [pltpu.VMEM((planes, *piece), F32)]
    )
    other = shifted(own, "core", 1)

    last = pl.BlockSpec((step // width, planes, share, width), lambda j: (steps, 0, 0, 0))
    update = pl.pallas_call(
        update_kernel,
        grid=(steps,),
        in_specs=[SMEM, part, part, last, last, blocked, blocked],
        out_specs=blocked,
        out_shape=jax.ShapeDtypeStruct((groups, planes, share, width), F32),
        scratch_shapes=[pltpu.VMEM((planes * share, lead), BF16)] * 2,
        cost_estimate=cost(flops(planes * share, lead, columns), 1 << 22),
        name="update",
    )(place, own, other, keep, keep_other, keep, keep_other)
    arrived = lax.all_to_all(
        update.reshape(groups * planes, share, width), ("x", "yl", "z"), 0, 0, tiled=True
    )
    sol = pl.pallas_call(
        finish_kernel,
        grid=(steps,),
        in_specs=[SMEM, part, part, pl.BlockSpec((rows, step), lambda j: (0, steps)), tall],
        out_specs=tall,
        out_shape=jax.ShapeDtypeStruct((rows, columns), F32),
        scratch_shapes=[pltpu.VMEM((rows, lead), BF16)] * 2,
        cost_estimate=cost(flops(rows, lead, columns), 1 << 23),
        name="finish",
    )(place, own, other, leaf, leaf)

    group = lax.axis_index(("x", "yl"))
    own_rows = lax.dynamic_slice_in_dim(anc_inverse, (z * cores + core) * share, share, 0)
    own_cols = lax.dynamic_slice_in_dim(anc_rhs, group * width, width, 1)
    anc_block = pl.pallas_call(
        total_kernel,
        out_shape=jax.ShapeDtypeStruct((share, width), F32),
        cost_estimate=cost(flops(share, anc, width), 1 << 21),
        name="total",
    )(own_rows, own_cols, arrived)
    spread = lax.all_to_all(
        jnp.broadcast_to(anc_block[None], (groups, share, width)), ("x", "yl"), 0, 0, tiled=True
    )
    return sol, jnp.moveaxis(spread, 0, 1).reshape(share, columns)


def solution(mesh):
    split = Mesh(
        mesh.devices.reshape(4, 2, 4, 2, mesh.shape["rhs"]), ("x", "yl", "z", "core", "rhs")
    )
    in_specs = (
        P(GRID_ROW, "rhs"),
        P(GRID_ROW),
        P(GRID_ROW, None),
        P(GRID_ROW, None),
        P(GRID_ROW, None),
        P(GRID_ROW),
        P(None, "rhs"),
        P(),
    )
    out_specs = (P(GRID_ROW, "rhs"), P(("z", "core"), "rhs"))
    return jax.shard_map(body, mesh=split, in_specs=in_specs, out_specs=out_specs, check_vma=False)
```

```python
import jax
import jax.numpy as jnp
from jax import lax
from jax.experimental import pallas as pl
from jax.experimental.pallas import tpu as pltpu
from jax.sharding import Mesh
from jax.sharding import PartitionSpec as P

F32 = jnp.float32
BF16 = jnp.bfloat16
GRID_ROW = ("x", "yl", "z", "core")


def shifted(array, axis, by, sources=None):
    devices = lax.axis_size(axis)
    pairs = [(i, (i + by) % devices) for i in range(devices)]
    if sources is not None:
        pairs = [pair for pair in pairs if pair[0] in sources]
    return lax.ppermute(array, axis, pairs)


def halves(a):
    high = a.astype(BF16)
    return high, (a - high.astype(F32)).astype(BF16)


def mxu(a, b):
    return jnp.dot(a, b, preferred_element_type=F32)


def dot3(a, b):
    return mxu(a[0], b[0]) + (mxu(a[0], b[1]) + mxu(a[1], b[0]))


def flops(m, k, n):
    return 6 * m * k * n


def cost(n_flops, n_bytes):
    return pl.CostEstimate(flops=n_flops, transcendentals=0, bytes_accessed=n_bytes)


SMEM = pl.BlockSpec(memory_space=pltpu.SMEM)
VMEM = pl.BlockSpec(memory_space=pltpu.VMEM)
LIMIT = pltpu.CompilerParams(vmem_limit_bytes=20 << 20)


def near(array):
    return pltpu.with_memory_space_constraint(array, pltpu.VMEM)


def small(kernel, place, arrays, outs, scratch=(), n_flops=1 << 20):
    return pl.pallas_call(
        kernel,
        in_specs=[SMEM] + [VMEM] * len(arrays),
        out_specs=[VMEM] * len(outs),
        out_shape=[pltpu.VMEM(shape, F32) for shape in outs],
        scratch_shapes=list(scratch),
        cost_estimate=cost(n_flops, 1 << 20),
        compiler_params=LIMIT,
    )(place, *[near(a) for a in arrays])


def lead_kernel(place, size, inverse, lower, rhs, a_out, keep_out, send_out):
    rows = lax.broadcasted_iota(jnp.int32, inverse.shape, 0)
    s = halves(jnp.where(rows < size[0], inverse[...], 0.0))
    a_out[...] = dot3(s, halves(lower[...]))
    half = rhs.shape[1] // 2
    first = dot3(s, halves(rhs[:, :half]))
    second = dot3(s, halves(rhs[:, half:]))
    own_first = place[1] == 0
    keep_out[...] = jnp.where(own_first, first, second)
    send_out[...] = jnp.where(own_first, second, first)


def merge_kernel(place, a_own, a_other, b_own, b_other, o0, o1, o2, o3, a_out, quarters):
    z, low = place[0], place[1] == 0
    a_low = jnp.where(low, a_own[...], a_other[...])
    a_high = halves(jnp.where(low, a_other[...], a_own[...]))
    b_low = jnp.where(low, b_own[...], b_other[...])
    b_high = jnp.where(low, b_other[...], b_own[...])
    tall = a_out.shape[0]
    rows = tuple(jnp.where(low, part[:tall], part[tall:]) for part in a_high)
    a_out[...] = dot3(rows, halves(a_low))
    merged = b_high - dot3(a_high, halves(b_low))
    count, _, width = quarters.shape
    for i in range(count):
        quarters[i] = merged[:, i * width : (i + 1) * width]
    for s, out in enumerate((o0, o1, o2, o3)):
        out[...] = quarters[lax.rem(z + s, count)]


def pick_kernel(place, a0, a1, a2, a3, out, mats):
    z = place[0]
    count = mats.shape[0]
    for s, a in enumerate((a0, a1, a2, a3)):
        mats[lax.rem(z + count - s, count)] = a[...]
    for i in range(out.shape[0]):
        out[i] = mats[i + 1]


def solve_kernel(place, r0, r1, r2, r3, m_own, m_other, o0, o1, o2, o3, bs, ends):
    z, low = place[0], place[1] == 0
    count = bs.shape[0]
    for s, r in enumerate((r0, r1, r2, r3)):
        bs[lax.rem(z + count - s, count)] = r[...]
    ends[0] = jnp.zeros(ends.shape[1:], F32)
    carried = bs[0]
    ends[1] = carried
    tall = m_own.shape[1]
    for i in range(1, count - 1):
        right = halves(carried)
        top = halves(jnp.where(low, m_own[i - 1], m_other[i - 1]))
        bottom = halves(jnp.where(low, m_other[i - 1], m_own[i - 1]))
        ends[i + 1, :tall] = bs[i, :tall] + dot3(top, right)
        ends[i + 1, tall:] = bs[i, tall:] + dot3(bottom, right)
        carried = ends[i + 1]
    for s, out in enumerate((o0, o1, o2, o3)):
        out[...] = ends[lax.rem(z + s, count)]


def gather_kernel(place, t0, t1, t2, t3, out, quarters):
    z = place[0]
    count, _, width = quarters.shape
    for s, t in enumerate((t0, t1, t2, t3)):
        quarters[lax.rem(z + count - s, count)] = t[...]
    for i in range(count):
        out[:, i * width : (i + 1) * width] = quarters[i]


def weigh_kernel(rows, inverse, coupling, after, m_high, m_low, hot):
    anc, touched = hot.shape
    at = lax.broadcasted_iota(jnp.int32, (anc, touched), 0)
    hot[...] = jnp.where(at == rows[...], 1.0, 0.0).astype(BF16)
    right = halves(coupling[...])
    block = anc // 3
    for i in range(3):
        span = slice(i * block, (i + 1) * block)
        reach, cols = (i + 1) * block, min(touched, (i + 1) * block)
        high, low = halves(inverse[span, :reach])
        picked = hot[:reach, :cols]
        g = halves(mxu(high, picked) + mxu(low, picked))
        m = dot3(g, tuple(part[:cols] for part in right))
        m_high[span], m_low[span] = halves(m)


def columns_of(step, width):
    return pl.ds(pl.multiple_of(step * width, width), width)


def leaf_kernel(
    place, size, inverse, lower, rhs, b_first, b_second, a_low, after, out, sh, sl, lh, ll, t
):
    step, last = pl.program_id(0), pl.num_programs(0) - 1
    high_core = place[1] == 1
    width = t.shape[1]

    @pl.when(step == 0)
    def _():
        rows = lax.broadcasted_iota(jnp.int32, inverse.shape, 0)
        sh[...], sl[...] = halves(jnp.where(rows < size[0], inverse[...], 0.0))
        lh[...], ll[...] = halves(lower[...])

    @pl.when(step < last)
    def _():
        cols = columns_of(lax.rem(step, last // 2), width)
        entering = jnp.where(step < last // 2, b_first[:, cols], b_second[:, cols])
        entering = jnp.where(high_core, entering, 0.0)
        t[...] = rhs[...] - dot3((lh[...], ll[...]), halves(entering))

    @pl.when(step == last)
    def _():
        t[...] = jnp.where(
            high_core, -dot3((lh[...], ll[...]), halves(a_low[...])), lower[...]
        )

    right = halves(t[...])
    block = inverse.shape[0] // 3
    cols = columns_of(step, width)
    for i in range(3):
        span, reach = slice(i * block, (i + 1) * block), (i + 1) * block
        out[span, cols] = dot3(
            (sh[span, :reach], sl[span, :reach]), (right[0][:reach], right[1][:reach])
        )


def couple_kernel(place, m_high, m_low, leaf, after, keep, send):
    low = place[1] == 0
    step = pl.program_id(0)
    planes, share, width = keep.shape[1:]
    wide = leaf.shape[1] // pl.num_programs(0)
    value = dot3((m_high[...], m_low[...]), halves(leaf[:, columns_of(step, wide)]))
    groups = wide // width
    for g in range(groups):
        cols = slice(g * width, (g + 1) * width)
        for p in range(planes):
            top = value[2 * p * share : (2 * p + 1) * share, cols]
            bottom = value[(2 * p + 1) * share : (2 * p + 2) * share, cols]
            keep[step * groups + g, p] = jnp.where(low, top, bottom)
            send[step * groups + g, p] = jnp.where(low, bottom, top)


def entering_chip(place, own, other, step, width):
    per = own.shape[1] // width
    cols = columns_of(lax.rem(step, per), width)
    return halves(jnp.where(step // per == place[1], own[:, cols], other[:, cols]))


def update_kernel(place, own, other, keep, arrived, out):
    groups, planes, share, width = out.shape
    tall, wide = planes * share, own.shape[0]
    per = wide // width
    added = [(keep[groups + g] + arrived[groups + g]).reshape(tall, width) for g in range(per)]
    n = halves(jnp.concatenate(added, axis=1))
    for step in range(groups // per):
        moved = dot3(n, entering_chip(place, own, other, jnp.int32(step), wide))
        for g in range(per):
            at = step * per + g
            c = (keep[at] + arrived[at]).reshape(tall, width)
            out[at] = (c - moved[:, g * width : (g + 1) * width]).reshape(planes, share, width)


def finish_kernel(place, own, other, leaf, sol, hh, hl):
    step = pl.program_id(0)
    width = sol.shape[1]

    @pl.when(step == 0)
    def _():
        hh[...], hl[...] = halves(leaf[:, pl.num_programs(0) * width :])

    carried = entering_chip(place, own, other, step, width)
    sol[...] = leaf[:, columns_of(step, width)] - dot3((hh[...], hl[...]), carried)


def total_kernel(own_rows, own_cols, arrived, out):
    total = arrived[0]
    for i in range(1, arrived.shape[0]):
        total = total + arrived[i]
    block = dot3(halves(own_rows[...]), halves(own_cols[...])) - total
    for g in range(out.shape[0]):
        out[g] = block


def whole_body(leaf_rhs, block_sizes, leaf_lower, leaf_inverse, coupling, anc_rows, anc_rhs, anc_inverse):
    rows, columns = leaf_rhs.shape
    lead = leaf_lower.shape[1]
    anc, touched = anc_inverse.shape[0], anc_rows.shape[0]
    planes, cores = lax.axis_size("z"), lax.axis_size("core")
    groups = lax.axis_size("x") * lax.axis_size("yl")
    z, core = lax.axis_index("z"), lax.axis_index("core")
    place = jnp.stack([z, core]).astype(jnp.int32)
    half, quarter = columns // cores, columns // (cores * planes)
    share, width = anc // (planes * cores), columns // groups
    piece = (lead, quarter)

    block = lambda r, c: pl.BlockSpec((r, c), lambda i: (0, 0))
    a_own, b_own, b_send = pl.pallas_call(
        lead_kernel,
        grid=(1,),
        in_specs=[SMEM, SMEM, block(lead, lead), block(lead, lead), block(lead, columns)],
        out_specs=[VMEM] * 3,
        out_shape=[pltpu.VMEM((lead, w), F32) for w in (lead, half, half)],
        cost_estimate=cost(flops(lead, lead, lead + columns), 1 << 21),
        name="lead",
    )(place, block_sizes, leaf_inverse, leaf_lower, leaf_rhs)
    a_other = shifted(a_own, "core", 1)
    b_other = shifted(b_send, "core", 1)
    b_low = shifted(b_own, "core", 1, (0,))

    m_high, m_low = pl.pallas_call(
        weigh_kernel,
        in_specs=[VMEM] * 4,
        out_specs=[VMEM] * 2,
        out_shape=[pltpu.VMEM((anc, rows), BF16)] * 2,
        scratch_shapes=[pltpu.VMEM((anc, touched), BF16)],
        cost_estimate=cost(flops(anc, touched, rows + anc), 1 << 22),
        compiler_params=LIMIT,
        name="weigh",
    )(anc_rows[None], anc_inverse, coupling, near(a_own))

    *blocks, a_pair = small(
        merge_kernel,
        place,
        (a_own, a_other, b_own, b_other),
        [piece] * 4 + [(lead // cores, lead)],
        [pltpu.VMEM((planes, *piece), F32)],
        flops(lead, lead, half + lead),
    )
    mats = [a_pair] + [shifted(a_pair, "z", s, (1, 2)) for s in range(1, planes)]
    blocks = [blocks[0]] + [shifted(blocks[s], "z", s, (0, 1, 2)) for s in range(1, planes)]

    mat_shape = (planes - 2, lead // cores, lead)
    (mats_own,) = small(
        pick_kernel, place, mats, [mat_shape], [pltpu.VMEM((planes, *mat_shape[1:]), F32)]
    )
    mats_other = shifted(mats_own, "core", 1)

    step = 2 * width
    steps = columns // step
    whole = lambda r, c: pl.BlockSpec((r, c), lambda j: (0, 0), pipeline_mode=pl.Buffered(1))
    leaf = pl.pallas_call(
        leaf_kernel,
        grid=(steps + 1,),
        in_specs=[
            SMEM,
            SMEM,
            whole(rows, rows),
            whole(rows, lead),
            pl.BlockSpec((rows, step), lambda j: (0, jnp.minimum(j, steps - 1))),
        ]
        + [VMEM] * 4,
        out_specs=VMEM,
        out_shape=pltpu.VMEM((rows, columns + lead), F32),
        scratch_shapes=[pltpu.VMEM((rows, rows), BF16)] * 2
        + [pltpu.VMEM((rows, lead), BF16)] * 2
        + [pltpu.VMEM((rows, step), F32)],
        cost_estimate=cost(flops(rows, rows, columns), 1 << 23),
        compiler_params=LIMIT,
        name="leaf",
    )(
        place,
        block_sizes,
        leaf_inverse,
        leaf_lower,
        leaf_rhs,
        *[near(a) for a in (b_low, b_other, a_other, mats_own)],
    )

    ends = small(
        solve_kernel,
        place,
        (*blocks, mats_own, mats_other),
        [piece] * 4,
        [pltpu.VMEM((planes, *piece), F32)] * 2,
        flops(lead, lead, 2 * quarter),
    )
    wide = (columns + lead) // width
    keep, send = pl.pallas_call(
        couple_kernel,
        grid=(steps + 1,),
        in_specs=[SMEM] + [VMEM] * 4,
        out_specs=[VMEM] * 2,
        out_shape=[pltpu.VMEM((wide, planes, share, width), F32)] * 2,
        cost_estimate=cost(flops(anc, rows, columns + lead), 1 << 23),
        compiler_params=LIMIT,
        name="couple",
    )(place, *[near(a) for a in (m_high, m_low, leaf, ends[0])])
    keep_other = shifted(send, "core", 1)
    ends = [ends[0]] + [shifted(ends[s], "z", s) for s in range(1, planes)]
    (own,) = small(gather_kernel, place, ends, [(lead, half)], [pltpu.VMEM((planes, *piece), F32)])
    other = shifted(own, "core", 1)

    (update,) = small(
        update_kernel,
        place,
        (own, other, keep, keep_other),
        [(groups, planes, share, width)],
        (),
        flops(planes * share, lead, columns),
    )
    arrived = lax.all_to_all(
        update.reshape(groups * planes, share, width), ("x", "yl", "z"), 0, 0, tiled=True
    )
    sol = pl.pallas_call(
        finish_kernel,
        grid=(steps,),
        in_specs=[SMEM] + [VMEM] * 3,
        out_specs=pl.BlockSpec((rows, step), lambda j: (0, j)),
        out_shape=jax.ShapeDtypeStruct((rows, columns), F32),
        scratch_shapes=[pltpu.VMEM((rows, lead), BF16)] * 2,
        cost_estimate=cost(flops(rows, lead, columns), 1 << 23),
        compiler_params=LIMIT,
        name="finish",
    )(place, near(own), near(other), near(leaf))

    group = lax.axis_index(("x", "yl"))
    own_rows = lax.dynamic_slice_in_dim(anc_inverse, (z * cores + core) * share, share, 0)
    own_cols = lax.dynamic_slice_in_dim(anc_rhs, group * width, width, 1)
    anc_blocks = pl.pallas_call(
        total_kernel,
        in_specs=[VMEM] * 3,
        out_specs=VMEM,
        out_shape=pltpu.VMEM((groups, share, width), F32),
        cost_estimate=cost(flops(share, anc, width), 1 << 21),
        compiler_params=LIMIT,
        name="total",
    )(own_rows, own_cols, near(arrived))
    spread = lax.all_to_all(anc_blocks, ("x", "yl"), 0, 0, tiled=True)
    return sol, jnp.moveaxis(spread, 0, 1).reshape(share, columns)


def solution(mesh):
    split = Mesh(
        mesh.devices.reshape(4, 2, 4, 2, mesh.shape["rhs"]), ("x", "yl", "z", "core", "rhs")
    )
    in_specs = (
        P(GRID_ROW, "rhs"),
        P(GRID_ROW),
        P(GRID_ROW, None),
        P(GRID_ROW, None),
        P(GRID_ROW, None),
        P(GRID_ROW),
        P(None, "rhs"),
        P(),
    )
    out_specs = (P(GRID_ROW, "rhs"), P(("z", "core"), "rhs"))
    return jax.shard_map(whole_body, mesh=split, in_specs=in_specs, out_specs=out_specs, check_vma=False)
```

```python
import jax
import jax.numpy as jnp
from jax import lax
from jax.experimental import pallas as pl
from jax.experimental.pallas import tpu as pltpu
from jax.sharding import Mesh
from jax.sharding import PartitionSpec as P

F32 = jnp.float32
BF16 = jnp.bfloat16
GRID_ROW = ("x", "yl", "z", "core")


def shifted(array, axis, by, sources=None):
    devices = lax.axis_size(axis)
    pairs = [(i, (i + by) % devices) for i in range(devices)]
    if sources is not None:
        pairs = [pair for pair in pairs if pair[0] in sources]
    return lax.ppermute(array, axis, pairs)


def exchanged(blocks, axes):
    return lax.all_to_all(blocks, axes, 0, 0, tiled=True)


def halves(a):
    high = a.astype(BF16)
    return high, (a - high.astype(F32)).astype(BF16)


def mxu(a, b):
    return jnp.dot(a, b, preferred_element_type=F32)


def dot3(a, b):
    return mxu(a[0], b[0]) + (mxu(a[0], b[1]) + mxu(a[1], b[0]))


def flops(m, k, n):
    return 6 * m * k * n


def cost(n_flops, n_bytes):
    return pl.CostEstimate(flops=n_flops, transcendentals=0, bytes_accessed=n_bytes)


SMEM = pl.BlockSpec(memory_space=pltpu.SMEM)
VMEM = pl.BlockSpec(memory_space=pltpu.VMEM)
LIMIT = pltpu.CompilerParams(vmem_limit_bytes=20 << 20)


def near(array):
    return pltpu.with_memory_space_constraint(array, pltpu.VMEM)


def far(array):
    return pltpu.with_memory_space_constraint(array, pltpu.HBM)


def whole(shape):
    return pl.BlockSpec(shape, lambda j: (0,) * len(shape), pipeline_mode=pl.Buffered(1))


def small(kernel, place, arrays, out, n_flops=1 << 20):
    return pl.pallas_call(
        kernel,
        grid=(1,),
        in_specs=[SMEM] + [VMEM] * len(arrays),
        out_specs=VMEM,
        out_shape=out,
        cost_estimate=cost(n_flops, 1 << 20),
        compiler_params=LIMIT,
    )(place, *arrays)


def lead_kernel(place, size, inverse, lower, rhs, a_out, b_out, send):
    rows = lax.broadcasted_iota(jnp.int32, inverse.shape, 0)
    s = halves(jnp.where(rows < size[0], inverse[...], 0.0))
    lead, half = inverse.shape[1], rhs.shape[1] // 2
    a = dot3(s, halves(lower[...]))
    a_out[...] = a
    send[:, :lead] = a
    first = dot3(s, halves(rhs[:, :half]))
    second = dot3(s, halves(rhs[:, half:]))
    own_first = place[1] == 0
    b_out[...] = jnp.where(own_first, first, second)
    send[:, lead:] = jnp.where(own_first, second, first)


def merge_kernel(place, a_own, b_own, other, out):
    low = place[1] == 0
    lead = a_own.shape[1]
    a_low = jnp.where(low, a_own[...], other[:, :lead])
    a_high = halves(jnp.where(low, other[:, :lead], a_own[...]))
    b_low = jnp.where(low, b_own[...], other[:, lead:])
    b_high = jnp.where(low, other[:, lead:], b_own[...])
    planes, tall, wide = out.shape
    half, width = tall // 2, wide // 2
    rows = tuple(jnp.where(low, part[:half], part[half:]) for part in a_high)
    mat = dot3(rows, halves(a_low))
    merged = b_high - dot3(a_high, halves(b_low))
    for i in range(planes):
        out[i, :, :width] = merged[:, i * width : (i + 1) * width]
        out[i, :half, width:] = mat[:, :width]
        out[i, half:, width:] = mat[:, width:]


def pick_kernel(place, blocks, out):
    width = out.shape[2]
    for i in range(out.shape[0]):
        out[i] = blocks[i + 1, :, width:]


def solve_kernel(place, blocks, m_own, m_other, out):
    low = place[1] == 0
    planes, _, width = out.shape
    half = m_own.shape[1] // 2
    out[0] = jnp.zeros(out.shape[1:], F32)
    carried = blocks[0, :, :width]
    out[1] = carried
    for i in range(1, planes - 1):
        right = halves(carried)
        for part in range(2):
            mine = low if part == 0 else jnp.logical_not(low)
            mat = jnp.where(mine, m_own[i - 1], m_other[i - 1])
            rows = slice(part * half, (part + 1) * half)
            moved = dot3(halves(mat[:half]), tuple(r[:width] for r in right))
            moved += dot3(halves(mat[half:]), tuple(r[width:] for r in right))
            out[i + 1, rows] = blocks[i, rows, :width] + moved
        carried = out[i + 1]


def weigh_kernel(rows, inverse, coupling, m_high, m_low, hot):
    anc, touched = hot.shape
    at = lax.broadcasted_iota(jnp.int32, (anc, touched), 0)
    hot[...] = jnp.where(at == rows[...], 1.0, 0.0).astype(BF16)
    right = halves(coupling[...])
    block = anc // 3
    for i in range(3):
        span = slice(i * block, (i + 1) * block)
        reach, cols = (i + 1) * block, min(touched, (i + 1) * block)
        high, low = halves(inverse[span, :reach])
        picked = hot[:reach, :cols]
        g = halves(mxu(high, picked) + mxu(low, picked))
        m = dot3(g, tuple(part[:cols] for part in right))
        m_high[span], m_low[span] = halves(m)


def columns_of(step, width):
    return pl.ds(pl.multiple_of(step * width, width), width)


def leaf_kernel(
    place, size, inverse, lower, rhs, b_first, other, out, sh, sl, lh, ll, t
):
    step, last = pl.program_id(0), pl.num_programs(0) - 1
    high_core = place[1] == 1
    width = t.shape[1]

    @pl.when(step == 0)
    def _():
        rows = lax.broadcasted_iota(jnp.int32, inverse.shape, 0)
        sh[...], sl[...] = halves(jnp.where(rows < size[0], inverse[...], 0.0))
        lh[...], ll[...] = halves(lower[...])

    @pl.when(step < last)
    def _():
        at = lax.rem(step, last // 2)
        second = other[:, columns_of(at + 1, width)]
        entering = jnp.where(step < last // 2, b_first[:, columns_of(at, width)], second)
        entering = jnp.where(high_core, entering, 0.0)
        t[...] = rhs[...] - dot3((lh[...], ll[...]), halves(entering))

    @pl.when(step == last)
    def _():
        t[...] = jnp.where(
            high_core, -dot3((lh[...], ll[...]), halves(other[:, :width])), lower[...]
        )

    right = halves(t[...])
    block = inverse.shape[0] // 3
    for i in range(3):
        span, reach = slice(i * block, (i + 1) * block), (i + 1) * block
        out[span] = dot3(
            (sh[span, :reach], sl[span, :reach]), (right[0][:reach], right[1][:reach])
        )


def couple_kernel(place, m_high, m_low, leaf, keep, send):
    low = place[1] == 0
    groups, planes, share, width = keep.shape
    value = dot3((m_high[...], m_low[...]), halves(leaf[...]))
    for g in range(groups):
        cols = slice(g * width, (g + 1) * width)
        for p in range(planes):
            top = value[2 * p * share : (2 * p + 1) * share, cols]
            bottom = value[(2 * p + 1) * share : (2 * p + 2) * share, cols]
            keep[g, p] = jnp.where(low, top, bottom)
            send[g, p] = jnp.where(low, bottom, top)


def entering_chip(place, own, other, step, width):
    planes, _, quarter = own.shape
    per = width // quarter
    half = planes // per
    first = lax.rem(step, half) * per
    mine = step // half == place[1]
    parts = [jnp.where(mine, own[first + i], other[first + i]) for i in range(per)]
    return halves(jnp.concatenate(parts, axis=1))


def update_kernel(place, own, other, n_keep, n_arrived, keep, arrived, out, nh, nl):
    groups, planes, share, width = out.shape
    tall = planes * share

    @pl.when(pl.program_id(0) == 0)
    def _():
        for g in range(groups):
            cols = slice(g * width, (g + 1) * width)
            n = (n_keep[g] + n_arrived[g]).reshape(tall, width)
            nh[:, cols], nl[:, cols] = halves(n)

    carried = entering_chip(place, own, other, pl.program_id(0), groups * width)
    moved = dot3((nh[...], nl[...]), carried)
    for g in range(groups):
        c = (keep[g] + arrived[g]).reshape(tall, width)
        out[g] = (c - moved[:, g * width : (g + 1) * width]).reshape(planes, share, width)


def finish_kernel(place, own, other, h, f, sol, hh, hl):
    step = pl.program_id(0)

    @pl.when(step == 0)
    def _():
        hh[...], hl[...] = halves(h[...])

    carried = entering_chip(place, own, other, step, sol.shape[1])
    sol[...] = f[...] - dot3((hh[...], hl[...]), carried)


def total_kernel(own_rows, own_cols, arrived, out):
    total = arrived[0]
    for i in range(1, arrived.shape[0]):
        total = total + arrived[i]
    block = dot3(halves(own_rows[...]), halves(own_cols[...])) - total
    for g in range(out.shape[0]):
        out[g] = block


def whole_body(leaf_rhs, block_sizes, leaf_lower, leaf_inverse, coupling, anc_rows, anc_rhs, anc_inverse):
    rows, columns = leaf_rhs.shape
    lead = leaf_lower.shape[1]
    anc, touched = anc_inverse.shape[0], anc_rows.shape[0]
    planes, cores = lax.axis_size("z"), lax.axis_size("core")
    groups = lax.axis_size("x") * lax.axis_size("yl")
    z, core = lax.axis_index("z"), lax.axis_index("core")
    place = jnp.stack([z, core]).astype(jnp.int32)
    half, quarter = columns // cores, columns // (cores * planes)
    share, width = anc // (planes * cores), columns // groups

    block = lambda r, c: whole((r, c))
    a_own, b_own, send = pl.pallas_call(
        lead_kernel,
        grid=(1,),
        in_specs=[SMEM, SMEM, block(lead, lead), block(lead, lead), block(lead, columns)],
        out_specs=[VMEM] * 3,
        out_shape=[pltpu.VMEM((lead, w), F32) for w in (lead, half, lead + half)],
        cost_estimate=cost(flops(lead, lead, lead + columns), 1 << 21),
        compiler_params=LIMIT,
        name="lead",
    )(place, block_sizes, far(leaf_inverse), far(leaf_lower), far(leaf_rhs))
    other = shifted(send, "core", 1)
    blocks = small(
        merge_kernel,
        place,
        (near(a_own), near(b_own), near(other)),
        pltpu.HBM((planes, lead, 2 * quarter), F32),
        flops(lead, lead, half + lead // cores),
    )
    blocks = exchanged(blocks, "z")
    b_low = shifted(b_own, "core", 1, (0,))
    mat_shape = (planes - 2, lead, lead // cores)
    mats_own = small(pick_kernel, place, (far(blocks),), pltpu.VMEM(mat_shape, F32))
    mats_other = shifted(mats_own, "core", 1)

    m_high, m_low = pl.pallas_call(
        weigh_kernel,
        out_shape=[pltpu.HBM((anc, rows), BF16)] * 2,
        scratch_shapes=[pltpu.VMEM((anc, touched), BF16)],
        cost_estimate=cost(flops(anc, touched, rows + anc), 1 << 22),
        compiler_params=LIMIT,
        name="weigh",
    )(anc_rows[None], far(anc_inverse), far(coupling))

    step = 2 * width
    steps = columns // step
    tall = pl.BlockSpec((rows, step), lambda j: (0, j))
    blocked = pl.BlockSpec((step // width, planes, share, width), lambda j: (j, 0, 0, 0))
    last = pl.BlockSpec((step // width, planes, share, width), lambda j: (steps, 0, 0, 0))
    leaf = pl.pallas_call(
        leaf_kernel,
        grid=(steps + 1,),
        in_specs=[
            SMEM,
            SMEM,
            whole((rows, rows)),
            whole((rows, lead)),
            pl.BlockSpec((rows, step), lambda j: (0, jnp.minimum(j, steps - 1))),
            whole(b_low.shape),
            whole(other.shape),
        ],
        out_specs=tall,
        out_shape=pltpu.HBM((rows, columns + lead), F32),
        scratch_shapes=[pltpu.VMEM((rows, rows), BF16)] * 2
        + [pltpu.VMEM((rows, lead), BF16)] * 2
        + [pltpu.VMEM((rows, step), F32)],
        cost_estimate=cost(flops(rows, rows, columns), 1 << 23),
        compiler_params=LIMIT,
        name="leaf",
    )(
        place,
        block_sizes,
        far(leaf_inverse),
        far(leaf_lower),
        far(leaf_rhs),
        far(b_low),
        far(other),
    )

    ends = small(
        solve_kernel,
        place,
        (far(blocks), near(mats_own), near(mats_other)),
        pltpu.HBM((planes, lead, quarter), F32),
        flops(lead, lead, 2 * quarter),
    )
    own = exchanged(ends, "z")
    own_other = shifted(own, "core", 1)
    wide = (columns + lead) // width
    keep, send = pl.pallas_call(
        couple_kernel,
        grid=(steps + 1,),
        in_specs=[SMEM, whole((anc, rows)), whole((anc, rows)), tall],
        out_specs=[blocked] * 2,
        out_shape=[pltpu.HBM((wide, planes, share, width), F32)] * 2,
        cost_estimate=cost(flops(anc, rows, columns + lead), 1 << 23),
        compiler_params=LIMIT,
        name="couple",
    )(place, far(m_high), far(m_low), far(leaf))
    keep_other = shifted(send, "core", 1)
    ends_spec = whole((planes, lead, quarter))
    update = pl.pallas_call(
        update_kernel,
        grid=(steps,),
        in_specs=[SMEM, ends_spec, ends_spec, last, last, blocked, blocked],
        out_specs=blocked,
        out_shape=pltpu.HBM((groups, planes, share, width), F32),
        scratch_shapes=[pltpu.VMEM((planes * share, lead), BF16)] * 2,
        cost_estimate=cost(flops(planes * share, lead, columns), 1 << 22),
        compiler_params=LIMIT,
        name="update",
    )(place, far(own), near(own_other), *[far(a) for a in (keep, keep_other)] * 2)
    update = update.reshape(groups * planes, share, width)
    arrived = exchanged(update, ("x", "yl", "z"))
    sol = pl.pallas_call(
        finish_kernel,
        grid=(steps,),
        in_specs=[SMEM, ends_spec, ends_spec, pl.BlockSpec((rows, step), lambda j: (0, steps)), tall],
        out_specs=tall,
        out_shape=jax.ShapeDtypeStruct((rows, columns), F32),
        scratch_shapes=[pltpu.VMEM((rows, lead), BF16)] * 2,
        cost_estimate=cost(flops(rows, lead, columns), 1 << 23),
        compiler_params=LIMIT,
        name="finish",
    )(place, far(own), far(own_other), far(leaf), far(leaf))

    group = lax.axis_index(("x", "yl"))
    own_rows = lax.dynamic_slice_in_dim(anc_inverse, (z * cores + core) * share, share, 0)
    own_cols = lax.dynamic_slice_in_dim(anc_rhs, group * width, width, 1)
    anc_blocks = pl.pallas_call(
        total_kernel,
        in_specs=[VMEM] * 3,
        out_specs=VMEM,
        out_shape=pltpu.VMEM((groups, share, width), F32),
        cost_estimate=cost(flops(share, anc, width), 1 << 21),
        compiler_params=LIMIT,
        name="total",
    )(own_rows, own_cols, near(arrived))
    spread = exchanged(anc_blocks, ("x", "yl"))
    return sol, jnp.moveaxis(spread, 0, 1).reshape(share, columns)


def solution(mesh):
    split = Mesh(
        mesh.devices.reshape(4, 2, 4, 2, mesh.shape["rhs"]), ("x", "yl", "z", "core", "rhs")
    )
    in_specs = (
        P(GRID_ROW, "rhs"),
        P(GRID_ROW),
        P(GRID_ROW, None),
        P(GRID_ROW, None),
        P(GRID_ROW, None),
        P(GRID_ROW),
        P(None, "rhs"),
        P(),
    )
    out_specs = (P(GRID_ROW, "rhs"), P(("z", "core"), "rhs"))
    return jax.shard_map(whole_body, mesh=split, in_specs=in_specs, out_specs=out_specs, check_vma=False)
```

```python
import jax
import jax.numpy as jnp
from jax import lax
from jax.experimental import pallas as pl
from jax.experimental.pallas import tpu as pltpu
from jax.sharding import Mesh
from jax.sharding import PartitionSpec as P

F32 = jnp.float32
BF16 = jnp.bfloat16
GRID_ROW = ("x", "yl", "z", "core")


def shifted(array, axis, by, sources=None):
    devices = lax.axis_size(axis)
    pairs = [(i, (i + by) % devices) for i in range(devices)]
    if sources is not None:
        pairs = [pair for pair in pairs if pair[0] in sources]
    return lax.ppermute(array, axis, pairs)


def exchanged(blocks, axes):
    return lax.all_to_all(blocks, axes, 0, 0, tiled=True)


def swapped(blocks):
    return [blocks[0]] + [shifted(b, "z", s) for s, b in enumerate(blocks) if s]


def halves(a):
    high = a.astype(BF16)
    return high, (a - high.astype(F32)).astype(BF16)


def mxu(a, b):
    return jnp.dot(a, b, preferred_element_type=F32)


def dot3(a, b):
    return mxu(a[0], b[0]) + (mxu(a[0], b[1]) + mxu(a[1], b[0]))


def flops(m, k, n):
    return 6 * m * k * n


def cost(n_flops, n_bytes):
    return pl.CostEstimate(flops=n_flops, transcendentals=0, bytes_accessed=n_bytes)


SMEM = pl.BlockSpec(memory_space=pltpu.SMEM)
VMEM = pl.BlockSpec(memory_space=pltpu.VMEM)
LIMIT = pltpu.CompilerParams(vmem_limit_bytes=20 << 20)


def near(array):
    return pltpu.with_memory_space_constraint(array, pltpu.VMEM)


def far(array):
    return pltpu.with_memory_space_constraint(array, pltpu.HBM)


def whole(shape):
    return pl.BlockSpec(shape, lambda j: (0,) * len(shape), pipeline_mode=pl.Buffered(1))


def small(kernel, place, arrays, outs, scratch=(), n_flops=1 << 20):
    return pl.pallas_call(
        kernel,
        in_specs=[SMEM] + [VMEM] * len(arrays),
        out_specs=[VMEM] * len(outs),
        out_shape=[pltpu.VMEM(shape, F32) for shape in outs],
        scratch_shapes=list(scratch),
        cost_estimate=cost(n_flops, 1 << 20),
        compiler_params=LIMIT,
    )(place, *[near(a) for a in arrays])


def lead_kernel(place, size, inverse, lower, rhs, a_out, b_out, send):
    rows = lax.broadcasted_iota(jnp.int32, inverse.shape, 0)
    s = halves(jnp.where(rows < size[0], inverse[...], 0.0))
    lead, half = inverse.shape[1], rhs.shape[1] // 2
    a = dot3(s, halves(lower[...]))
    a_out[...] = a
    send[:, :lead] = a
    first = dot3(s, halves(rhs[:, :half]))
    second = dot3(s, halves(rhs[:, half:]))
    own_first = place[1] == 0
    b_out[...] = jnp.where(own_first, first, second)
    send[:, lead:] = jnp.where(own_first, second, first)


def merge_kernel(place, a_own, b_own, other, o0, o1, o2, o3, quarters):
    z, low = place[0], place[1] == 0
    lead = a_own.shape[1]
    a_low = jnp.where(low, a_own[...], other[:, :lead])
    a_high = halves(jnp.where(low, other[:, :lead], a_own[...]))
    b_low = jnp.where(low, b_own[...], other[:, lead:])
    b_high = jnp.where(low, other[:, lead:], b_own[...])
    planes, tall, width = quarters.shape
    half = tall // 2
    rows = tuple(jnp.where(low, part[:half], part[half:]) for part in a_high)
    mat = dot3(rows, halves(a_low))
    merged = b_high - dot3(a_high, halves(b_low))
    for i in range(planes):
        quarters[i] = merged[:, i * width : (i + 1) * width]
    for s, out in enumerate((o0, o1, o2, o3)):
        out[:, :width] = quarters[lax.rem(z + s, planes)]
        out[:half, width:] = mat[:, :width]
        out[half:, width:] = mat[:, width:]


def pick_kernel(place, r0, r1, r2, r3, out, mats):
    planes, _, width = mats.shape
    for s, r in enumerate((r0, r1, r2, r3)):
        mats[lax.rem(place[0] + planes - s, planes)] = r[:, width:]
    for i in range(out.shape[0]):
        out[i] = mats[i + 1]


def solve_kernel(place, r0, r1, r2, r3, m_own, m_other, o0, o1, o2, o3, blocks, ends):
    z, low = place[0], place[1] == 0
    planes, _, width = ends.shape
    half = m_own.shape[1] // 2
    for s, r in enumerate((r0, r1, r2, r3)):
        blocks[lax.rem(z + planes - s, planes)] = r[:, :width]
    ends[0] = jnp.zeros(ends.shape[1:], F32)
    carried = blocks[0]
    ends[1] = carried
    for i in range(1, planes - 1):
        right = halves(carried)
        for part in range(2):
            mine = low if part == 0 else jnp.logical_not(low)
            mat = jnp.where(mine, m_own[i - 1], m_other[i - 1])
            rows = slice(part * half, (part + 1) * half)
            moved = dot3(halves(mat[:half]), tuple(r[:width] for r in right))
            moved += dot3(halves(mat[half:]), tuple(r[width:] for r in right))
            ends[i + 1, rows] = blocks[i, rows] + moved
        carried = ends[i + 1]
    for s, out in enumerate((o0, o1, o2, o3)):
        out[...] = ends[lax.rem(z + s, planes)]


def gather_kernel(place, t0, t1, t2, t3, out):
    planes = out.shape[0]
    for s, t in enumerate((t0, t1, t2, t3)):
        out[lax.rem(place[0] + planes - s, planes)] = t[...]


def weigh_kernel(rows, inverse, coupling, m_high, m_low, hot):
    anc, touched = hot.shape
    at = lax.broadcasted_iota(jnp.int32, (anc, touched), 0)
    hot[...] = jnp.where(at == rows[...], 1.0, 0.0).astype(BF16)
    right = halves(coupling[...])
    block = anc // 3
    for i in range(3):
        span = slice(i * block, (i + 1) * block)
        reach, cols = (i + 1) * block, min(touched, (i + 1) * block)
        high, low = halves(inverse[span, :reach])
        picked = hot[:reach, :cols]
        g = halves(mxu(high, picked) + mxu(low, picked))
        m = dot3(g, tuple(part[:cols] for part in right))
        m_high[span], m_low[span] = halves(m)


def columns_of(step, width):
    return pl.ds(pl.multiple_of(step * width, width), width)


def leaf_kernel(
    place, size, inverse, lower, rhs, b_first, other, out, sh, sl, lh, ll, t
):
    step, last = pl.program_id(0), pl.num_programs(0) - 1
    high_core = place[1] == 1
    width = t.shape[1]

    @pl.when(step == 0)
    def _():
        rows = lax.broadcasted_iota(jnp.int32, inverse.shape, 0)
        sh[...], sl[...] = halves(jnp.where(rows < size[0], inverse[...], 0.0))
        lh[...], ll[...] = halves(lower[...])

    @pl.when(step < last)
    def _():
        at = lax.rem(step, last // 2)
        second = other[:, columns_of(at + 1, width)]
        entering = jnp.where(step < last // 2, b_first[:, columns_of(at, width)], second)
        entering = jnp.where(high_core, entering, 0.0)
        t[...] = rhs[...] - dot3((lh[...], ll[...]), halves(entering))

    @pl.when(step == last)
    def _():
        t[...] = jnp.where(
            high_core, -dot3((lh[...], ll[...]), halves(other[:, :width])), lower[...]
        )

    right = halves(t[...])
    block = inverse.shape[0] // 3
    cols = columns_of(step, width)
    for i in range(3):
        span, reach = slice(i * block, (i + 1) * block), (i + 1) * block
        out[span, cols] = dot3(
            (sh[span, :reach], sl[span, :reach]), (right[0][:reach], right[1][:reach])
        )


def couple_kernel(place, m_high, m_low, leaf, keep, send):
    low = place[1] == 0
    step = pl.program_id(0)
    planes, share, width = keep.shape[1:]
    wide = leaf.shape[1] // pl.num_programs(0)
    value = dot3((m_high[...], m_low[...]), halves(leaf[:, columns_of(step, wide)]))
    groups = wide // width
    for g in range(groups):
        cols = slice(g * width, (g + 1) * width)
        for p in range(planes):
            top = value[2 * p * share : (2 * p + 1) * share, cols]
            bottom = value[(2 * p + 1) * share : (2 * p + 2) * share, cols]
            keep[step * groups + g, p] = jnp.where(low, top, bottom)
            send[step * groups + g, p] = jnp.where(low, bottom, top)


def entering_chip(place, own, other, step, width):
    planes, _, quarter = own.shape
    per = width // quarter
    half = planes // per
    first = lax.rem(step, half) * per
    mine = step // half == place[1]
    parts = [jnp.where(mine, own[first + i], other[first + i]) for i in range(per)]
    return halves(jnp.concatenate(parts, axis=1))


def update_kernel(place, own, other, keep, arrived, out, nh, nl):
    groups, planes, share, width = out.shape
    tall, step, steps = planes * share, pl.program_id(0), pl.num_programs(0)

    @pl.when(step == 0)
    def _():
        for g in range(groups):
            cols = slice(g * width, (g + 1) * width)
            n = (keep[steps * groups + g] + arrived[steps * groups + g]).reshape(tall, width)
            nh[:, cols], nl[:, cols] = halves(n)

    carried = entering_chip(place, own, other, step, groups * width)
    moved = dot3((nh[...], nl[...]), carried)
    for g in range(groups):
        c = (keep[step * groups + g] + arrived[step * groups + g]).reshape(tall, width)
        out[g] = (c - moved[:, g * width : (g + 1) * width]).reshape(planes, share, width)


def finish_kernel(place, own, other, leaf, sol, hh, hl):
    step = pl.program_id(0)
    width = sol.shape[1]

    @pl.when(step == 0)
    def _():
        hh[...], hl[...] = halves(leaf[:, pl.num_programs(0) * width :])

    carried = entering_chip(place, own, other, step, width)
    sol[...] = leaf[:, columns_of(step, width)] - dot3((hh[...], hl[...]), carried)


def right_kernel(rows, cols, out):
    out[...] = dot3(halves(rows[...]), halves(cols[...]))


def total_kernel(right, arrived, out, total):
    step = pl.program_id(0)
    part = arrived[0]
    for i in range(1, arrived.shape[0]):
        part = part + arrived[i]

    @pl.when(step == 0)
    def _():
        total[...] = right[...] - part

    @pl.when(step > 0)
    def _():
        total[...] = total[...] - part

    @pl.when(step == pl.num_programs(0) - 1)
    def _():
        for g in range(out.shape[0]):
            out[g] = total[...]


def whole_body(leaf_rhs, block_sizes, leaf_lower, leaf_inverse, coupling, anc_rows, anc_rhs, anc_inverse):
    rows, columns = leaf_rhs.shape
    lead = leaf_lower.shape[1]
    anc, touched = anc_inverse.shape[0], anc_rows.shape[0]
    planes, cores = lax.axis_size("z"), lax.axis_size("core")
    groups = lax.axis_size("x") * lax.axis_size("yl")
    z, core = lax.axis_index("z"), lax.axis_index("core")
    place = jnp.stack([z, core]).astype(jnp.int32)
    half, quarter = columns // cores, columns // (cores * planes)
    share, width = anc // (planes * cores), columns // groups

    block = lambda r, c: pl.BlockSpec((r, c), lambda i: (0, 0))
    a_own, b_own, send = pl.pallas_call(
        lead_kernel,
        grid=(1,),
        in_specs=[SMEM, SMEM, block(lead, lead), block(lead, lead), block(lead, columns)],
        out_specs=[VMEM] * 3,
        out_shape=[pltpu.VMEM((lead, w), F32) for w in (lead, half, lead + half)],
        cost_estimate=cost(flops(lead, lead, lead + columns), 1 << 21),
        compiler_params=LIMIT,
        name="lead",
    )(place, block_sizes, far(leaf_inverse), far(leaf_lower), far(leaf_rhs))
    other = shifted(send, "core", 1)
    blocks = small(
        merge_kernel,
        place,
        (a_own, b_own, other),
        [(lead, 2 * quarter)] * planes,
        [pltpu.VMEM((planes, lead, quarter), F32)],
        flops(lead, lead, half + lead // cores),
    )
    blocks = swapped(blocks)
    b_low = shifted(b_own, "core", 1, (0,))
    held = pltpu.VMEM((planes, lead, quarter), F32)
    mat_shape = (planes - 2, lead, lead // cores)
    (mats_own,) = small(pick_kernel, place, blocks, [mat_shape], [held])
    mats_other = shifted(mats_own, "core", 1)

    m_high, m_low = pl.pallas_call(
        weigh_kernel,
        in_specs=[VMEM] * 3,
        out_specs=[VMEM] * 2,
        out_shape=[pltpu.VMEM((anc, rows), BF16)] * 2,
        scratch_shapes=[pltpu.VMEM((anc, touched), BF16)],
        cost_estimate=cost(flops(anc, touched, rows + anc), 1 << 22),
        compiler_params=LIMIT,
        name="weigh",
    )(anc_rows[None], anc_inverse, coupling)

    step = 2 * width
    steps = columns // step
    leaf = pl.pallas_call(
        leaf_kernel,
        grid=(steps + 1,),
        in_specs=[
            SMEM,
            SMEM,
            whole((rows, rows)),
            whole((rows, lead)),
            pl.BlockSpec((rows, step), lambda j: (0, jnp.minimum(j, steps - 1))),
        ]
        + [VMEM] * 2,
        out_specs=VMEM,
        out_shape=pltpu.VMEM((rows, columns + lead), F32),
        scratch_shapes=[pltpu.VMEM((rows, rows), BF16)] * 2
        + [pltpu.VMEM((rows, lead), BF16)] * 2
        + [pltpu.VMEM((rows, step), F32)],
        cost_estimate=cost(flops(rows, rows, columns), 1 << 23),
        compiler_params=LIMIT,
        name="leaf",
    )(
        place,
        block_sizes,
        leaf_inverse,
        leaf_lower,
        leaf_rhs,
        *[near(a) for a in (b_low, other)],
    )

    ends = small(
        solve_kernel,
        place,
        (*blocks, mats_own, mats_other),
        [(lead, quarter)] * planes,
        [held, held],
        flops(lead, lead, 2 * quarter),
    )
    arrivals = swapped(ends)
    (own,) = small(gather_kernel, place, arrivals, [(planes, lead, quarter)])
    own_other = shifted(own, "core", 1)
    wide = (columns + lead) // width
    keep, send = pl.pallas_call(
        couple_kernel,
        grid=(steps + 1,),
        in_specs=[SMEM] + [VMEM] * 3,
        out_specs=[VMEM] * 2,
        out_shape=[pltpu.VMEM((wide, planes, share, width), F32)] * 2,
        cost_estimate=cost(flops(anc, rows, columns + lead), 1 << 23),
        compiler_params=LIMIT,
        name="couple",
    )(place, *[near(a) for a in (m_high, m_low, leaf)])
    keep_other = shifted(send, "core", 1)
    update = pl.pallas_call(
        update_kernel,
        grid=(steps,),
        in_specs=[SMEM] + [VMEM] * 4,
        out_specs=pl.BlockSpec((step // width, planes, share, width), lambda j: (j, 0, 0, 0)),
        out_shape=pltpu.HBM((groups, planes, share, width), F32),
        scratch_shapes=[pltpu.VMEM((planes * share, lead), BF16)] * 2,
        cost_estimate=cost(flops(planes * share, lead, columns), 1 << 22),
        compiler_params=LIMIT,
        name="update",
    )(place, *[near(a) for a in (own, own_other, keep, keep_other)])
    update = update.reshape(groups * planes, share, width)
    arrived = exchanged(update, ("x", "yl", "z"))
    sol = pl.pallas_call(
        finish_kernel,
        grid=(steps,),
        in_specs=[SMEM] + [VMEM] * 3,
        out_specs=pl.BlockSpec((rows, step), lambda j: (0, j)),
        out_shape=jax.ShapeDtypeStruct((rows, columns), F32),
        scratch_shapes=[pltpu.VMEM((rows, lead), BF16)] * 2,
        cost_estimate=cost(flops(rows, lead, columns), 1 << 23),
        compiler_params=LIMIT,
        name="finish",
    )(place, near(own), near(own_other), near(leaf))

    group = lax.axis_index(("x", "yl"))
    own_rows = lax.dynamic_slice_in_dim(anc_inverse, (z * cores + core) * share, share, 0)
    own_cols = lax.dynamic_slice_in_dim(anc_rhs, group * width, width, 1)
    right = pl.pallas_call(
        right_kernel,
        out_shape=pltpu.HBM((share, width), F32),
        cost_estimate=cost(flops(share, anc, width), 1 << 20),
        compiler_params=LIMIT,
        name="right",
    )(own_rows, own_cols)
    anc_blocks = pl.pallas_call(
        total_kernel,
        grid=(planes,),
        in_specs=[whole((share, width)), pl.BlockSpec((groups, share, width), lambda j: (j, 0, 0))],
        out_specs=VMEM,
        out_shape=pltpu.VMEM((groups, share, width), F32),
        scratch_shapes=[pltpu.VMEM((share, width), F32)],
        cost_estimate=cost(1 << 20, 1 << 21),
        compiler_params=LIMIT,
        name="total",
    )(far(right), far(arrived))
    spread = exchanged(anc_blocks, ("x", "yl"))
    return sol, jnp.moveaxis(spread, 0, 1).reshape(share, columns)


def solution(mesh):
    split = Mesh(
        mesh.devices.reshape(4, 2, 4, 2, mesh.shape["rhs"]), ("x", "yl", "z", "core", "rhs")
    )
    in_specs = (
        P(GRID_ROW, "rhs"),
        P(GRID_ROW),
        P(GRID_ROW, None),
        P(GRID_ROW, None),
        P(GRID_ROW, None),
        P(GRID_ROW),
        P(None, "rhs"),
        P(),
    )
    out_specs = (P(GRID_ROW, "rhs"), P(("z", "core"), "rhs"))
    return jax.shard_map(whole_body, mesh=split, in_specs=in_specs, out_specs=out_specs, check_vma=False)
```

```python
import functools

import jax
import jax.numpy as jnp
from jax import lax
from jax.experimental import pallas as pl
from jax.experimental.pallas import tpu as pltpu
from jax.sharding import Mesh
from jax.sharding import PartitionSpec as P

F32 = jnp.float32
BF16 = jnp.bfloat16
GRID_ROW = ("x", "yl", "z", "core")


def shifted(array, axis, by, sources=None):
    devices = lax.axis_size(axis)
    pairs = [(i, (i + by) % devices) for i in range(devices)]
    if sources is not None:
        pairs = [pair for pair in pairs if pair[0] in sources]
    return lax.ppermute(array, axis, pairs)


def exchanged(blocks, axes):
    return lax.all_to_all(blocks, axes, 0, 0, tiled=True)


def swapped(blocks):
    return [blocks[0]] + [shifted(b, "z", s) for s, b in enumerate(blocks) if s]


def halves(a):
    high = a.astype(BF16)
    return high, (a - high.astype(F32)).astype(BF16)


def mxu(a, b):
    return jnp.dot(a, b, preferred_element_type=F32)


def dot3(a, b):
    return mxu(a[0], b[0]) + (mxu(a[0], b[1]) + mxu(a[1], b[0]))


def flops(m, k, n):
    return 6 * m * k * n


def cost(n_flops, n_bytes):
    return pl.CostEstimate(flops=n_flops, transcendentals=0, bytes_accessed=n_bytes)


SMEM = pl.BlockSpec(memory_space=pltpu.SMEM)
VMEM = pl.BlockSpec(memory_space=pltpu.VMEM)
LIMIT = pltpu.CompilerParams(vmem_limit_bytes=20 << 20)


def near(array):
    return pltpu.with_memory_space_constraint(array, pltpu.VMEM)


def far(array):
    return pltpu.with_memory_space_constraint(array, pltpu.HBM)


def whole(shape):
    return pl.BlockSpec(shape, lambda j: (0,) * len(shape), pipeline_mode=pl.Buffered(1))


def small(kernel, place, arrays, outs, scratch=(), n_flops=1 << 20):
    return pl.pallas_call(
        kernel,
        in_specs=[SMEM] + [VMEM] * len(arrays),
        out_specs=[VMEM] * len(outs),
        out_shape=[pltpu.VMEM(shape, F32) for shape in outs],
        scratch_shapes=list(scratch),
        cost_estimate=cost(n_flops, 1 << 20),
        compiler_params=LIMIT,
    )(place, *[near(a) for a in arrays])


def lead_kernel(place, size, inverse, lower, rhs, a_out, b_out, send):
    rows = lax.broadcasted_iota(jnp.int32, inverse.shape, 0)
    s = halves(jnp.where(rows < size[0], inverse[...], 0.0))
    lead, half = inverse.shape[1], rhs.shape[1] // 2
    a = dot3(s, halves(lower[...]))
    a_out[...] = a
    send[:, :lead] = a
    first = dot3(s, halves(rhs[:, :half]))
    second = dot3(s, halves(rhs[:, half:]))
    own_first = place[1] == 0
    b_out[...] = jnp.where(own_first, first, second)
    send[:, lead:] = jnp.where(own_first, second, first)


def merge_kernel(place, a_own, b_own, other, o0, o1, o2, o3, quarters):
    z, low = place[0], place[1] == 0
    lead = a_own.shape[1]
    a_low = jnp.where(low, a_own[...], other[:, :lead])
    a_high = halves(jnp.where(low, other[:, :lead], a_own[...]))
    b_low = jnp.where(low, b_own[...], other[:, lead:])
    b_high = jnp.where(low, other[:, lead:], b_own[...])
    planes, _, width = quarters.shape
    mat = dot3(a_high, halves(a_low))
    merged = b_high - dot3(a_high, halves(b_low))
    for i in range(planes):
        quarters[i] = merged[:, i * width : (i + 1) * width]
    for s, out in enumerate((o0, o1, o2, o3)):
        out[:, :width] = quarters[lax.rem(z + s, planes)]
        out[:, width:] = mat


def solve_kernel(place, r0, r1, r2, r3, o0, o1, o2, o3, blocks, mats, ends):
    z = place[0]
    planes, _, width = ends.shape
    for s, r in enumerate((r0, r1, r2, r3)):
        at = lax.rem(z + planes - s, planes)
        blocks[at] = r[:, :width]
        mats[at] = r[:, width:]
    ends[0] = jnp.zeros(ends.shape[1:], F32)
    carried = blocks[0]
    ends[1] = carried
    for i in range(1, planes - 1):
        carried = blocks[i] + dot3(halves(mats[i]), halves(carried))
        ends[i + 1] = carried
    for s, out in enumerate((o0, o1, o2, o3)):
        out[...] = ends[lax.rem(z + s, planes)]


def gather_kernel(place, t0, t1, t2, t3, out):
    planes = out.shape[0]
    for s, t in enumerate((t0, t1, t2, t3)):
        out[lax.rem(place[0] + planes - s, planes)] = t[...]


def weigh_kernel(rows, inverse, coupling, m_high, m_low, hot):
    anc, touched = hot.shape
    at = lax.broadcasted_iota(jnp.int32, (anc, touched), 0)
    hot[...] = jnp.where(at == rows[...], 1.0, 0.0).astype(BF16)
    right = halves(coupling[...])
    block = anc // 3
    for i in range(3):
        span = slice(i * block, (i + 1) * block)
        reach, cols = (i + 1) * block, min(touched, (i + 1) * block)
        high, low = halves(inverse[span, :reach])
        picked = hot[:reach, :cols]
        g = halves(mxu(high, picked) + mxu(low, picked))
        m = dot3(g, tuple(part[:cols] for part in right))
        m_high[span], m_low[span] = halves(m)


def columns_of(step, width):
    return pl.ds(pl.multiple_of(step * width, width), width)


def leaf_kernel(
    place, size, inverse, lower, rhs, b_first, other, out, sh, sl, lh, ll, t
):
    step, last = pl.program_id(0), pl.num_programs(0) - 1
    high_core = place[1] == 1
    width = t.shape[1]

    @pl.when(step == 0)
    def _():
        rows = lax.broadcasted_iota(jnp.int32, inverse.shape, 0)
        sh[...], sl[...] = halves(jnp.where(rows < size[0], inverse[...], 0.0))
        lh[...], ll[...] = halves(lower[...])

    @pl.when(step < last)
    def _():
        at = lax.rem(step, last // 2)
        second = other[:, columns_of(at + 1, width)]
        entering = jnp.where(step < last // 2, b_first[:, columns_of(at, width)], second)
        entering = jnp.where(high_core, entering, 0.0)
        t[...] = rhs[...] - dot3((lh[...], ll[...]), halves(entering))

    @pl.when(step == last)
    def _():
        t[...] = jnp.where(
            high_core, -dot3((lh[...], ll[...]), halves(other[:, :width])), lower[...]
        )

    right = halves(t[...])
    block = inverse.shape[0] // 3
    cols = columns_of(step, width)
    for i in range(3):
        span, reach = slice(i * block, (i + 1) * block), (i + 1) * block
        out[span, cols] = dot3(
            (sh[span, :reach], sl[span, :reach]), (right[0][:reach], right[1][:reach])
        )


def couple_kernel(first, place, m_high, m_low, leaf, keep, send):
    low = place[1] == 0
    step = pl.program_id(0)
    planes, share, width = keep.shape[1:]
    groups = keep.shape[0] // pl.num_programs(0)
    cols = columns_of(first + step, groups * width)
    value = dot3((m_high[...], m_low[...]), halves(leaf[:, cols]))
    for g in range(groups):
        cols = slice(g * width, (g + 1) * width)
        for p in range(planes):
            top = value[2 * p * share : (2 * p + 1) * share, cols]
            bottom = value[(2 * p + 1) * share : (2 * p + 2) * share, cols]
            keep[step * groups + g, p] = jnp.where(low, top, bottom)
            send[step * groups + g, p] = jnp.where(low, bottom, top)


def entering_chip(own, other, mine, first, width):
    quarter = own.shape[2]
    parts = [jnp.where(mine, own[first + i], other[first + i]) for i in range(width // quarter)]
    return halves(jnp.concatenate(parts, axis=1))


def update_kernel(place, source, n_keep, n_other, c_keep, c_other, *rest):
    out, nh, nl = rest[-3:]
    groups, planes, share, width = out.shape
    tall, step, steps = planes * share, pl.program_id(0), pl.num_programs(0)

    @pl.when(step == 0)
    def _():
        for g in range(groups):
            cols = slice(g * width, (g + 1) * width)
            nh[:, cols], nl[:, cols] = halves((n_keep[g] + n_other[g]).reshape(tall, width))

    own = len(rest) == 3
    half = place[1] if own else 1 - place[1]
    parts = [source[step * groups + i] for i in range(groups)]
    moved = dot3((nh[...], nl[...]), halves(jnp.concatenate(parts, axis=1)))
    for g in range(groups):
        at = (half * steps + step) * groups + g
        c = (c_keep[at] + c_other[at]).reshape(tall, width)
        out[g] = (c - moved[:, g * width : (g + 1) * width]).reshape(planes, share, width)


def finish_kernel(place, own, other, leaf, sol, hh, hl):
    step, steps = pl.program_id(0), pl.num_programs(0)
    width = sol.shape[1]

    @pl.when(step == 0)
    def _():
        hh[...], hl[...] = halves(leaf[:, steps * width :])

    mine = step // (steps // 2) == place[1]
    first = lax.rem(step, steps // 2) * (width // own.shape[2])
    carried = entering_chip(own, other, mine, first, width)
    sol[...] = leaf[:, columns_of(step, width)] - dot3((hh[...], hl[...]), carried)


def right_kernel(rows, cols, out):
    out[...] = dot3(halves(rows[...]), halves(cols[...]))


def total_kernel(right, arrived, out, buffer, sems):
    chunks = buffer.shape[0]
    size = buffer.shape[1]
    copies = [
        pltpu.make_async_copy(arrived.at[pl.ds(i * size, size)], buffer.at[i], sems.at[i])
        for i in range(chunks)
    ]
    for copy in copies:
        copy.start()
    total = right[...]
    for i, copy in enumerate(copies):
        copy.wait()
        for j in range(size):
            total = total - buffer[i, j]
    for g in range(out.shape[0]):
        out[g] = total


def lay_kernel(place, spread, out):
    groups, _, width = spread.shape
    low = place[1] == 0
    for g in range(groups):
        other = (g + groups // 2) % groups
        out[:, g * width : (g + 1) * width] = jnp.where(low, spread[g], spread[other])


def whole_body(leaf_rhs, block_sizes, leaf_lower, leaf_inverse, coupling, anc_rows, anc_rhs, anc_inverse):
    rows, columns = leaf_rhs.shape
    lead = leaf_lower.shape[1]
    anc, touched = anc_inverse.shape[0], anc_rows.shape[0]
    planes, cores = lax.axis_size("z"), lax.axis_size("core")
    groups = lax.axis_size("x") * lax.axis_size("yl")
    z, core = lax.axis_index("z"), lax.axis_index("core")
    place = jnp.stack([z, core]).astype(jnp.int32)
    half, quarter = columns // cores, columns // (cores * planes)
    share, width = anc // (planes * cores), columns // groups

    block = lambda r, c: pl.BlockSpec((r, c), lambda i: (0, 0))
    a_own, b_own, send = pl.pallas_call(
        lead_kernel,
        grid=(1,),
        in_specs=[SMEM, SMEM, block(lead, lead), block(lead, lead), block(lead, columns)],
        out_specs=[VMEM] * 3,
        out_shape=[pltpu.VMEM((lead, w), F32) for w in (lead, half, lead + half)],
        cost_estimate=cost(flops(lead, lead, lead + columns), 1 << 21),
        compiler_params=LIMIT,
        name="lead",
    )(place, block_sizes, far(leaf_inverse), far(leaf_lower), far(leaf_rhs))
    other = shifted(send, "core", 1)
    held = pltpu.VMEM((planes, lead, quarter), F32)
    blocks = small(
        merge_kernel,
        place,
        (a_own, b_own, other),
        [(lead, quarter + lead)] * planes,
        [held],
        flops(lead, lead, half + lead),
    )
    blocks = swapped(blocks)
    b_low = shifted(b_own, "core", 1, (0,))
    m_high, m_low = pl.pallas_call(
        weigh_kernel,
        in_specs=[VMEM] * 3,
        out_specs=[VMEM] * 2,
        out_shape=[pltpu.VMEM((anc, rows), BF16)] * 2,
        scratch_shapes=[pltpu.VMEM((anc, touched), BF16)],
        cost_estimate=cost(flops(anc, touched, rows + anc), 1 << 22),
        compiler_params=LIMIT,
        name="weigh",
    )(anc_rows[None], anc_inverse, coupling)

    step = 2 * width
    steps = columns // step
    leaf = pl.pallas_call(
        leaf_kernel,
        grid=(steps + 1,),
        in_specs=[
            SMEM,
            SMEM,
            whole((rows, rows)),
            whole((rows, lead)),
            pl.BlockSpec((rows, step), lambda j: (0, jnp.minimum(j, steps - 1))),
        ]
        + [VMEM] * 2,
        out_specs=VMEM,
        out_shape=pltpu.VMEM((rows, columns + lead), F32),
        scratch_shapes=[pltpu.VMEM((rows, rows), BF16)] * 2
        + [pltpu.VMEM((rows, lead), BF16)] * 2
        + [pltpu.VMEM((rows, step), F32)],
        cost_estimate=cost(flops(rows, rows, columns), 1 << 23),
        compiler_params=LIMIT,
        name="leaf",
    )(
        place,
        block_sizes,
        leaf_inverse,
        leaf_lower,
        leaf_rhs,
        *[near(a) for a in (b_low, other)],
    )

    def couple(first, count):
        return pl.pallas_call(
            functools.partial(couple_kernel, first),
            grid=(count,),
            in_specs=[SMEM] + [VMEM] * 3,
            out_specs=[VMEM] * 2,
            out_shape=[pltpu.VMEM((count * step // width, planes, share, width), F32)] * 2,
            cost_estimate=cost(flops(anc, rows, count * step), 1 << 23),
            compiler_params=LIMIT,
        )(place, *[near(a) for a in (m_high, m_low, leaf)])

    n_keep, n_send = couple(steps, 1)
    n_other = shifted(n_send, "core", 1)
    ends = small(
        solve_kernel,
        place,
        blocks,
        [(lead, quarter)] * planes,
        [held, pltpu.VMEM((planes, lead, lead), F32), held],
        flops(lead, lead, 2 * quarter),
    )
    c_keep, c_send = couple(0, steps)
    c_other = shifted(c_send, "core", 1)
    arrivals = swapped(ends)
    (own,) = small(gather_kernel, place, arrivals, [(planes, lead, quarter)])
    own_other = shifted(own, "core", 1)

    def updated(source, ahead):
        sums = (n_keep, n_other, c_keep, c_other)
        first = len(ahead) * steps // 2
        return pl.pallas_call(
            update_kernel,
            grid=(steps // 2,),
            in_specs=[SMEM] + [VMEM] * 5 + [pl.BlockSpec(memory_space=pl.ANY)] * len(ahead),
            out_specs=pl.BlockSpec(
                (step // width, planes, share, width), lambda j: (first + j, 0, 0, 0)
            ),
            out_shape=pltpu.HBM((groups, planes, share, width), F32),
            input_output_aliases={6: 0} if ahead else {},
            scratch_shapes=[pltpu.VMEM((planes * share, lead), BF16)] * 2,
            cost_estimate=cost(flops(planes * share, lead, half), 1 << 22),
            compiler_params=LIMIT,
        )(place, near(source), *[near(a) for a in sums], *ahead)

    update = updated(own, ())
    update = updated(own_other, (update,))
    update = update.reshape(groups * planes, share, width)
    arrived = exchanged(update, ("x", "yl", "z"))
    sol = pl.pallas_call(
        finish_kernel,
        grid=(steps,),
        in_specs=[SMEM] + [VMEM] * 3,
        out_specs=pl.BlockSpec((rows, step), lambda j: (0, j)),
        out_shape=jax.ShapeDtypeStruct((rows, columns), F32),
        scratch_shapes=[pltpu.VMEM((rows, lead), BF16)] * 2,
        cost_estimate=cost(flops(rows, lead, columns), 1 << 23),
        compiler_params=LIMIT,
        name="finish",
    )(place, near(own), near(own_other), near(leaf))

    group = lax.rem(lax.axis_index(("x", "yl")) + core * (groups // 2), groups)
    own_rows = lax.dynamic_slice_in_dim(anc_inverse, (z * cores + core) * share, share, 0)
    own_cols = lax.dynamic_slice_in_dim(anc_rhs, group * width, width, 1)
    right = pl.pallas_call(
        right_kernel,
        out_shape=pltpu.HBM((share, width), F32),
        cost_estimate=cost(flops(share, anc, width), 1 << 20),
        compiler_params=LIMIT,
        name="right",
    )(own_rows, own_cols)
    anc_blocks = pl.pallas_call(
        total_kernel,
        in_specs=[VMEM, pl.BlockSpec(memory_space=pl.ANY)],
        out_specs=VMEM,
        out_shape=pltpu.VMEM((groups, share, width), F32),
        scratch_shapes=[
            pltpu.VMEM((planes, groups, share, width), F32),
            pltpu.SemaphoreType.DMA((planes,)),
        ],
        cost_estimate=cost(1 << 20, 1 << 21),
        compiler_params=LIMIT,
        name="total",
    )(far(right), far(arrived))
    spread = exchanged(anc_blocks, ("x", "yl"))
    anc = pl.pallas_call(
        lay_kernel,
        in_specs=[SMEM, VMEM],
        out_specs=VMEM,
        out_shape=jax.ShapeDtypeStruct((share, columns), F32),
        cost_estimate=cost(1 << 18, 1 << 20),
        compiler_params=LIMIT,
        name="lay",
    )(place, near(spread))
    return sol, anc


def solution(mesh):
    split = Mesh(
        mesh.devices.reshape(4, 2, 4, 2, mesh.shape["rhs"]), ("x", "yl", "z", "core", "rhs")
    )
    in_specs = (
        P(GRID_ROW, "rhs"),
        P(GRID_ROW),
        P(GRID_ROW, None),
        P(GRID_ROW, None),
        P(GRID_ROW, None),
        P(GRID_ROW),
        P(None, "rhs"),
        P(),
    )
    out_specs = (P(GRID_ROW, "rhs"), P(("z", "core"), "rhs"))
    return jax.shard_map(whole_body, mesh=split, in_specs=in_specs, out_specs=out_specs, check_vma=False)
```
